128 devices in a mesh: freq: 64 (over z, y, x_hi, core), kpt: 2 (over x_lo).
Axes of the slice: x: 4 (x_hi: 2, x_lo: 2; x = x_hi * 2 + x_lo), y: 4, z: 4, core: 2. Of those that a mesh axis runs over, the one named last changes fastest.
Arguments:
- band_energy: float32 [2, 384], P('kpt'), may hold values from -4.5 to 4.5, as said below
- projector: bfloat16 [2, 640, 384], P('kpt', 'freq'), may hold values from -0.25 to 0.25
- sigma: float32 [2, 5, 5, 128, 64], P(None, None, None, 'freq'), may hold values from -8.5 to 8.5, as said below
- atom_of_slot: int32 [128], replicated, may hold values from 0 to 127, each once
- kweight: int32 [2], replicated, may hold values from 1 to 16
Outputs:
- local_green: float32 [2, 5, 5, 128, 64], P(None, None, None, ('freq', 'kpt'))
The draws below stay inside these ranges and needn't reach their ends.
Inputs may be any that keep to these rules, and one draw needn't show every extreme that they name: `band_energy`: every entry is a band energy; the energies of one k-point share a common offset drawn per k-point. Each block sigma[0, :, :, s, n] is symmetric; each block sigma[1, :, :, s, n] is symmetric and negative definite. `atom_of_slot`: A permutation of 0 to 127; slot s belongs to the owner s // (128 // 64) along freq.
All inputs are finite; a program needn't handle non-finite values.
Results may differ from the reference program's by a relative error of at most 0.0003.
Values may be sent and summed in bfloat16 or wider, within the bound.
No kernel may reach another device: no remote copies, remote signals or barrier semaphores. Data moves between devices by JAX's collectives and lax.ppermute only.
A program may use at most 64 MiB of HBM per device.

```python
import math
import jax
import jax.numpy as jnp
from jax import lax

BANDS = 384
ATOMS = 128
ORBS = 5
ORBITALS = 640
KPOINTS = 2
FREQS = 64


def draw_band_energy(key, part):
    first, second = jax.random.split(jax.random.fold_in(key, 11))
    offset = jax.random.uniform(first, (KPOINTS, 1), jnp.float32, -2.0, 2.0)
    base = jax.random.uniform(second, (KPOINTS, BANDS), jnp.float32, -2.5, 2.5)
    return (offset + base).astype(jnp.float32)


def draw_sigma(key, part):
    first, second = jax.random.split(jax.random.fold_in(key, 23))
    shape = (ORBS, ORBS, ATOMS, FREQS)
    raw = jax.random.truncated_normal(first, -3.0, 3.0, shape, jnp.float32)
    factor = jax.random.truncated_normal(second, -3.0, 3.0, shape, jnp.float32)
    real_scale = 0.3
    imag_scale = 0.45
    real_part = real_scale * (raw + jnp.transpose(raw, (1, 0, 2, 3)))
    gram = jnp.einsum('mcaf,ocaf->moaf', factor, factor) / ORBS
    eye = jnp.eye(ORBS, dtype=jnp.float32)[:, :, None, None]
    imag_part = -(imag_scale * gram + 0.1 * eye)
    return jnp.stack([real_part, imag_part]).astype(jnp.float32)


def levels(key, dims, cuts, smallest, top_value):
    gain = 1.0
    for position, blocks in cuts:
        steps = jax.random.uniform(jax.random.fold_in(jax.random.fold_in(key, 6), position), (blocks,), jnp.float32, smallest / len(cuts), top_value / len(cuts))
        gain = gain * jnp.repeat(jnp.exp(steps), dims[position] // blocks).reshape((-1,) + (1,) * (len(dims) - 1 - position))
    return gain


def bell_draw(own_key, extent, width, reach, pieces=(), kind=jnp.bfloat16):
    entries = jax.random.normal(own_key, extent, jnp.float32) * width
    if len(pieces) > 0:
        entries = levels(own_key, extent, pieces, -0.22, 0.18) * entries
    return jnp.clip(entries, min=-reach, max=reach).astype(kind)


def setup_inputs(seed: int = 0) -> dict:
    key_of = jax.random.split(jax.random.key(seed), 6)
    band_energy = draw_band_energy(jax.random.fold_in(key_of[5], 71), 0)
    projector = bell_draw(key_of[1], (KPOINTS, ORBITALS, BANDS), ORBITALS ** -0.5, 0.25, ((0, 2), (1, 64)))
    sigma = draw_sigma(jax.random.fold_in(key_of[5], 71), 0)
    atom_of_slot = jax.random.permutation(key_of[3], ATOMS).astype(jnp.int32)
    kweight = jax.random.randint(key_of[4], (KPOINTS,), 1, 17).astype(jnp.int32)
    return dict(band_energy=band_energy, projector=projector, sigma=sigma, atom_of_slot=atom_of_slot, kweight=kweight)


HIGH = lax.Precision.HIGHEST
BETA_INV = 0.1

def local_block(energy, proj, real_sig, imag_sig, omega):
    proj3 = proj.reshape(ATOMS, ORBS, BANDS).astype(jnp.float32)
    real_rows = jnp.einsum('amo,aob->amb', real_sig, proj3, precision=HIGH).reshape(ATOMS * ORBS, BANDS).astype(jnp.bfloat16)
    imag_rows = jnp.einsum('amo,aob->amb', imag_sig, proj3, precision=HIGH).reshape(ATOMS * ORBS, BANDS).astype(jnp.bfloat16)
    up_real = jnp.dot(proj.T.astype(jnp.float32), real_rows.astype(jnp.float32), preferred_element_type=jnp.float32)
    up_imag = jnp.dot(proj.T.astype(jnp.float32), imag_rows.astype(jnp.float32), preferred_element_type=jnp.float32)
    eye = jnp.eye(BANDS, dtype=jnp.float32)
    x_mat = -jnp.diag(energy) - 0.5 * (up_real + up_real.T)
    y_mat = omega * eye - 0.5 * (up_imag + up_imag.T)
    lower = jnp.linalg.cholesky(y_mat)
    left = jax.scipy.linalg.solve_triangular(lower, x_mat, lower=True)
    core = jax.scipy.linalg.solve_triangular(lower, left.T, lower=True)
    core = 0.5 * (core + core.T)
    square = jnp.dot(core, core, precision=HIGH) + eye
    factor = jnp.linalg.cholesky(square)
    upper_rows = jax.scipy.linalg.solve_triangular(lower, proj.astype(jnp.float32).T, lower=True).T
    solved = jax.scipy.linalg.cho_solve((factor, True), upper_rows.T)
    wide = solved.T.reshape(ATOMS, ORBS, BANDS)
    turned = jnp.dot(upper_rows, core, precision=HIGH).reshape(ATOMS, ORBS, BANDS)
    real_part = jnp.einsum('amb,aob->amo', turned, wide, precision=HIGH)
    imag_part = -jnp.einsum('amb,aob->amo', upper_rows.reshape(ATOMS, ORBS, BANDS), wide, precision=HIGH)
    return jnp.stack([real_part, imag_part])

def reference(band_energy, projector, sigma, atom_of_slot, kweight):
    onehot = (atom_of_slot[:, None] == jnp.arange(ATOMS, dtype=jnp.int32)[None, :]).astype(jnp.float32)
    sig_atom = jnp.einsum('xmosf,sa->xmoaf', sigma, onehot, precision=HIGH)
    weights = kweight.astype(jnp.float32)
    total = jnp.sum(weights)

    def one_freq(index):
        omega = (2.0 * index.astype(jnp.float32) + 1.0) * math.pi * BETA_INV
        sig_now = lax.dynamic_index_in_dim(sig_atom, index, 4, keepdims=False)
        real_sig = jnp.transpose(sig_now[0], (2, 0, 1))
        imag_sig = jnp.transpose(sig_now[1], (2, 0, 1))

        def add_point(point, acc):
            block = local_block(band_energy[point], projector[point], real_sig, imag_sig, omega)
            return acc + weights[point] * block
        return lax.fori_loop(0, KPOINTS, add_point, jnp.zeros((2, ATOMS, ORBS, ORBS), jnp.float32))
    blocks = lax.map(one_freq, jnp.arange(FREQS, dtype=jnp.int32))
    slots = jnp.einsum('fxamo,sa->xmosf', blocks, onehot, precision=HIGH)
    return slots / total
```

```python
import math

import jax
import jax.numpy as jnp
from jax import lax
from jax.experimental import pallas as pl
from jax.experimental.pallas import tpu as pltpu
from jax.sharding import PartitionSpec as P

BANDS = 384
ATOMS = 128
ORBS = 5
PARTS = 2 * ORBS * ORBS
BETA_INV = 0.1
LANES = 128
CHUNKS = BANDS // LANES
ROWS = 8
PANELS = LANES // ROWS

f32 = jnp.float32
bf16 = jnp.bfloat16


def split3(x):
    hi = x.astype(bf16)
    rest = x - hi.astype(f32)
    mid = rest.astype(bf16)
    low = (rest - mid.astype(f32)).astype(bf16)
    return hi, mid, low


def pack_kernel(proj_ref, sig_ref, out_ref, tmp_ref):
    tmp_ref[...] = jnp.zeros_like(tmp_ref)
    tmp_ref[0:PARTS, 0:64] = sig_ref[:, 0, :]
    tmp_ref[64 : 64 + PARTS, 0:64] = sig_ref[:, 1, :]
    turned = tmp_ref[...].T
    hi, mid, low = split3(turned)
    parts = [hi.astype(f32), mid.astype(f32), low.astype(f32)]
    rows = lax.broadcasted_iota(jnp.int32, (16, LANES), 0)
    base = [
        jnp.concatenate(
            [proj_ref[:, LANES * c : LANES * (c + 1)].astype(f32), jnp.zeros((6, LANES), f32)], axis=0
        )
        for c in range(3)
    ]
    for n in range(64):
        for c in range(3):
            row = jnp.broadcast_to(parts[c][n : n + 1, :], (16, LANES))
            out_ref[n, :, LANES * c : LANES * (c + 1)] = jnp.where(rows == 10, row, base[c]).astype(bf16)


def unpack_kernel(in_ref, out_ref):
    both = in_ref[pl.ds(0, 64, stride=2), :] + in_ref[pl.ds(1, 64, stride=2), :]
    turned = both.T
    for i in range(PARTS):
        out_ref[i, :, :] = turned[i : i + 1, :]


def cmul(ar, ai, br, bi):
    return ar * br - ai * bi, ar * bi + ai * br


def row_of(x, i):
    return jnp.broadcast_to(x[i : i + 1, :], (ROWS, LANES))


def lane_of(x, i):
    return jnp.broadcast_to(x[:, i : i + 1], (ROWS, LANES))


def sweep_panel(j, diag, rest, sub_iota, lane_iota):
    first = ROWS * j
    cols = [(lane_of(diag[0], first + t), lane_of(diag[1], first + t)) for t in range(ROWS)]
    in_block = (lane_iota >= first) & (lane_iota < first + ROWS)
    eye = jnp.where(lane_iota == sub_iota + first, 1.0, 0.0).astype(f32)
    work = [(jnp.where(in_block, eye, diag[0]), jnp.where(in_block, 0.0, diag[1]))] + rest
    for p in range(0, ROWS, 2):
        q = p + 1
        ar, ai = row_of(cols[p][0], p), row_of(cols[p][1], p)
        br, bi = row_of(cols[q][0], p), row_of(cols[q][1], p)
        dr, di = row_of(cols[q][0], q), row_of(cols[q][1], q)
        adr, adi = cmul(ar, ai, dr, di)
        bbr, bbi = cmul(br, bi, br, bi)
        det_r, det_i = adr - bbr, adi - bbi
        inv = 1.0 / (det_r * det_r + det_i * det_i)
        vr, vi = det_r * inv, -(det_i * inv)
        w11 = cmul(dr, di, vr, vi)
        w22 = cmul(ar, ai, vr, vi)
        w12 = cmul(-br, -bi, vr, vi)
        cpr, cpi = cols[p]
        cqr, cqi = cols[q]
        t1, t2 = cmul(cpr, cpi, *w11), cmul(cqr, cqi, *w12)
        t3, t4 = cmul(cpr, cpi, *w12), cmul(cqr, cqi, *w22)
        at_p, at_q = sub_iota == p, sub_iota == q
        fp = [jnp.where(at_p, -w11[z], jnp.where(at_q, -w12[z], t1[z] + t2[z])) for z in range(2)]
        fq = [jnp.where(at_p, -w12[z], jnp.where(at_q, -w22[z], t3[z] + t4[z])) for z in range(2)]
        keep = ~(at_p | at_q)

        def step(x):
            xr, xi = x
            pr, pi = row_of(xr, p), row_of(xi, p)
            qr, qi = row_of(xr, q), row_of(xi, q)
            yr = jnp.where(keep, xr, 0.0) - (fp[0] * pr - fp[1] * pi) - (fq[0] * qr - fq[1] * qi)
            yi = jnp.where(keep, xi, 0.0) - (fp[0] * pi + fp[1] * pr) - (fq[0] * qi + fq[1] * qr)
            return yr, yi

        for t in range(q + 1, ROWS):
            cols[t] = step(cols[t])
        work = [step(x) for x in work]
    head_r, head_i = work[0]
    update = [(jnp.where(in_block, eye - head_r, head_r), jnp.where(in_block, -head_i, head_i))] + work[1:]
    final = [(jnp.where(in_block, -head_r, head_r), jnp.where(in_block, -head_i, head_i))] + work[1:]
    return update, final


def stack_parts(top, bottom, order):
    parts = split3(jnp.concatenate([top, bottom], axis=0))
    return jnp.concatenate([parts[i] for i in order], axis=0)


LEFT = (0, 0, 0, 1, 1, 2)
RIGHT = (0, 1, 2, 0, 1, 0)


def main_kernel(buf_ref, atom_ref, energy_ref, weight_ref, out_ref, re_ref, im_ref, rows_ref, out_tmp):
    freq = lax.axis_index("freq")
    kpt = lax.axis_index("kpt")
    omega = (2.0 * freq.astype(f32) + 1.0) * math.pi * BETA_INV
    total = (weight_ref[0] + weight_ref[1]).astype(f32)
    own = jnp.where(kpt == 0, weight_ref[0], weight_ref[1]).astype(f32)

    atom = atom_ref[...]
    base = (atom >> 1) * 16 + (atom & 1) * 5
    lane_row = lax.broadcasted_iota(jnp.int32, (1, LANES), 1)
    target = jnp.concatenate([base + o for o in range(ORBS)] + [(lane_row >> 1) * 16 + 10], axis=1)
    pick = (lax.broadcasted_iota(jnp.int32, (1024, 768), 0) == target).astype(f32).astype(bf16)
    turned = lax.dot_general(
        buf_ref[...], pick, (((0,), (0,)), ((), ())), preferred_element_type=f32
    )
    proj_t = [turned[:, LANES * o : LANES * (o + 1)] for o in range(ORBS)]
    sig_parts = turned[0:128, 640:768] + turned[128:256, 640:768] + turned[256:384, 640:768]
    odd = (lax.broadcasted_iota(jnp.int32, (64, LANES), 1) & 1) == 1
    sig = jnp.where(odd, sig_parts[64:128, :], sig_parts[0:64, :])

    proj_b = turned[:, 0:640].astype(bf16)
    for x in range(2):
        for m in range(ORBS):
            acc = None
            for o in range(ORBS):
                i = x * 25 + m * 5 + o
                term = sig[i : i + 1, :] * proj_t[o]
                acc = term if acc is None else acc + term
            rows_ref[x * BANDS : (x + 1) * BANDS, LANES * m : LANES * (m + 1)] = acc.astype(bf16)
    ups = lax.dot_general(
        rows_ref[...], proj_b, (((1,), (1,)), ((), ())), preferred_element_type=f32
    )
    up_r, up_i = ups[0:BANDS, :], ups[BANDS : 2 * BANDS, :]
    ii = lax.broadcasted_iota(jnp.int32, (BANDS, BANDS), 0)
    jj = lax.broadcasted_iota(jnp.int32, (BANDS, BANDS), 1)
    x_mat = jnp.where(ii == jj, -energy_ref[...], 0.0) - 0.5 * (up_r + up_r.T)
    y_mat = jnp.where(ii == jj, omega, 0.0) - 0.5 * (up_i + up_i.T)
    for c in range(CHUNKS):
        re_ref[c, :, :] = x_mat[:, LANES * c : LANES * (c + 1)]
        im_ref[c, :, :] = y_mat[:, LANES * c : LANES * (c + 1)]

    sub_iota = lax.broadcasted_iota(jnp.int32, (ROWS, LANES), 0)
    lane_iota = lax.broadcasted_iota(jnp.int32, (ROWS, LANES), 1)

    def block_step(kb, carry):
        chunk = [kb, lax.rem(kb + 1, CHUNKS), lax.rem(kb + 2, CHUNKS)]
        for j in range(PANELS):
            at = pl.ds(pl.multiple_of(kb * LANES + ROWS * j, ROWS), ROWS)
            panel = [(re_ref[c, at, :], im_ref[c, at, :]) for c in chunk]
            update, final = sweep_panel(j, panel[0], panel[1:], sub_iota, lane_iota)
            left = jnp.concatenate(
                [stack_parts(r, i, LEFT) for r, i in panel], axis=1
            )
            for z in range(CHUNKS):
                r, i = update[z]
                right = stack_parts(
                    jnp.concatenate([r, i], axis=1), jnp.concatenate([-i, r], axis=1), RIGHT
                )
                prod = lax.dot_general(left, right, (((0,), (0,)), ((), ())), preferred_element_type=f32)
                for y in range(CHUNKS):
                    here = pl.ds(pl.multiple_of(chunk[y] * LANES, LANES), LANES)
                    piece = prod[LANES * y : LANES * (y + 1), :]
                    re_ref[chunk[z], here, :] = re_ref[chunk[z], here, :] - piece[:, 0:LANES]
                    im_ref[chunk[z], here, :] = im_ref[chunk[z], here, :] - piece[:, LANES:]
            for z in range(CHUNKS):
                re_ref[chunk[z], at, :] = final[z][0]
                im_ref[chunk[z], at, :] = final[z][1]
        return carry

    lax.fori_loop(0, CHUNKS, block_step, 0)

    wide = []
    for ref in (re_ref, im_ref):
        full = jnp.concatenate([ref[c, :, :] for c in range(CHUNKS)], axis=1)
        hi = full.astype(bf16)
        low = (full - hi.astype(f32)).astype(bf16)
        wide.append(jnp.concatenate([hi, low], axis=1))
    left = jnp.concatenate(wide, axis=0)
    twice = jnp.concatenate([proj_b, proj_b], axis=0)
    gp = lax.dot_general(left, twice, (((1,), (0,)), ((), ())), preferred_element_type=f32)
    scale = -own / total
    out_tmp[...] = jnp.zeros_like(out_tmp)
    for x in range(2):
        for m in range(ORBS):
            v = gp[x * BANDS : (x + 1) * BANDS, LANES * m : LANES * (m + 1)]
            for o in range(m, ORBS):
                val = jnp.sum(v * proj_t[o], axis=0, keepdims=True) * scale
                i1, i2 = x * 25 + m * 5 + o, x * 25 + o * 5 + m
                out_tmp[i1 : i1 + 1, :] = val
                if o != m:
                    out_tmp[i2 : i2 + 1, :] = val
    out_ref[...] = out_tmp[...].T


def vmem():
    return pl.BlockSpec(memory_space=pltpu.VMEM)


def local(band_energy, projector, sigma, atom_of_slot, kweight):
    packed = pl.pallas_call(
        pack_kernel,
        out_shape=jax.ShapeDtypeStruct((64, 16, BANDS), bf16),
        in_specs=[vmem(), vmem()],
        out_specs=vmem(),
        scratch_shapes=[pltpu.VMEM((LANES, LANES), f32)],
        name="pack",
    )(projector.reshape(10, BANDS), sigma.reshape(PARTS, 2, 64))
    arrived = lax.all_to_all(packed, "freq", split_axis=0, concat_axis=0, tiled=True)
    blocks = pl.pallas_call(
        main_kernel,
        out_shape=jax.ShapeDtypeStruct((ATOMS, LANES), f32),
        in_specs=[vmem(), vmem(), vmem(), pl.BlockSpec(memory_space=pltpu.SMEM)],
        out_specs=vmem(),
        scratch_shapes=[
            pltpu.VMEM((CHUNKS, BANDS, LANES), f32),
            pltpu.VMEM((CHUNKS, BANDS, LANES), f32),
            pltpu.VMEM((2 * BANDS, 640), bf16),
            pltpu.VMEM((LANES, LANES), f32),
        ],
        name="green",
    )(arrived.reshape(1024, BANDS), atom_of_slot.reshape(1, ATOMS), band_energy, kweight)
    back = lax.all_to_all(
        blocks.reshape(ATOMS, 1, LANES), ("freq", "kpt"), split_axis=0, concat_axis=0, tiled=True
    )
    out = pl.pallas_call(
        unpack_kernel,
        out_shape=jax.ShapeDtypeStruct((PARTS, 1, 64), f32),
        in_specs=[vmem()],
        out_specs=vmem(),
        name="unpack",
    )(back.reshape(ATOMS, LANES))
    return out.reshape(2, ORBS, ORBS, 1, 64)


def solution(mesh):
    placed = (P("kpt", None), P("kpt", "freq", None), P(None, None, None, "freq", None), P(), P())
    return jax.shard_map(
        local,
        mesh=mesh,
        in_specs=placed,
        out_specs=P(None, None, None, ("freq", "kpt"), None),
        check_vma=False,
    )
```

```python
import math

import jax
import jax.numpy as jnp
from jax import lax
from jax.experimental import pallas as pl
from jax.experimental.pallas import tpu as pltpu
from jax.sharding import PartitionSpec as P

BANDS = 384
ATOMS = 128
ORBS = 5
PARTS = 2 * ORBS * ORBS
BETA_INV = 0.1
LANES = 128
CHUNKS = BANDS // LANES
ROWS = 8
GROUP = 2

f32 = jnp.float32
bf16 = jnp.bfloat16


def split3(x):
    hi = x.astype(bf16)
    rest = x - hi.astype(f32)
    mid = rest.astype(bf16)
    low = (rest - mid.astype(f32)).astype(bf16)
    return hi, mid, low


def pack_kernel(proj_ref, sig_ref, out_ref, tmp_ref):
    tmp_ref[...] = jnp.zeros_like(tmp_ref)
    tmp_ref[0:PARTS, 0:64] = sig_ref[:, 0, :]
    tmp_ref[64 : 64 + PARTS, 0:64] = sig_ref[:, 1, :]
    turned = tmp_ref[...].T
    hi, mid, low = split3(turned)
    parts = [hi.astype(f32), mid.astype(f32), low.astype(f32)]
    rows = lax.broadcasted_iota(jnp.int32, (16, LANES), 0)
    base = [
        jnp.concatenate(
            [proj_ref[:, LANES * c : LANES * (c + 1)].astype(f32), jnp.zeros((6, LANES), f32)], axis=0
        )
        for c in range(3)
    ]
    for n in range(64):
        for c in range(3):
            row = jnp.broadcast_to(parts[c][n : n + 1, :], (16, LANES))
            out_ref[n, :, LANES * c : LANES * (c + 1)] = jnp.where(rows == 10, row, base[c]).astype(bf16)


def unpack_kernel(in_ref, out_ref):
    both = in_ref[pl.ds(0, 64, stride=2), :] + in_ref[pl.ds(1, 64, stride=2), :]
    turned = both.T
    for i in range(PARTS):
        out_ref[i, :, :] = turned[i : i + 1, :]


def cmul(ar, ai, br, bi):
    return ar * br - ai * bi, ar * bi + ai * br


def row_of(x, i):
    return jnp.broadcast_to(x[i : i + 1, :], (ROWS, LANES))


def lane_of(x, i):
    return jnp.broadcast_to(x[:, i : i + 1], (ROWS, LANES))


def sweep_panel(panel, first, sub_iota, lane_iota):
    home, off = divmod(first, LANES)
    diag = panel[home]
    cols = [(lane_of(diag[0], off + t), lane_of(diag[1], off + t)) for t in range(ROWS)]
    in_block = (lane_iota >= off) & (lane_iota < off + ROWS)
    eye = jnp.where(lane_iota == sub_iota + off, 1.0, 0.0).astype(f32)
    work = list(panel)
    work[home] = (jnp.where(in_block, eye, diag[0]), jnp.where(in_block, 0.0, diag[1]))
    for p in range(0, ROWS, 2):
        q = p + 1
        ar, ai = row_of(cols[p][0], p), row_of(cols[p][1], p)
        br, bi = row_of(cols[q][0], p), row_of(cols[q][1], p)
        dr, di = row_of(cols[q][0], q), row_of(cols[q][1], q)
        adr, adi = cmul(ar, ai, dr, di)
        bbr, bbi = cmul(br, bi, br, bi)
        det_r, det_i = adr - bbr, adi - bbi
        inv = 1.0 / (det_r * det_r + det_i * det_i)
        vr, vi = det_r * inv, -(det_i * inv)
        w11 = cmul(dr, di, vr, vi)
        w22 = cmul(ar, ai, vr, vi)
        w12 = cmul(-br, -bi, vr, vi)
        cpr, cpi = cols[p]
        cqr, cqi = cols[q]
        t1, t2 = cmul(cpr, cpi, *w11), cmul(cqr, cqi, *w12)
        t3, t4 = cmul(cpr, cpi, *w12), cmul(cqr, cqi, *w22)
        at_p, at_q = sub_iota == p, sub_iota == q
        fp = [jnp.where(at_p, -w11[z], jnp.where(at_q, -w12[z], t1[z] + t2[z])) for z in range(2)]
        fq = [jnp.where(at_p, -w12[z], jnp.where(at_q, -w22[z], t3[z] + t4[z])) for z in range(2)]
        keep = ~(at_p | at_q)

        def step(x):
            xr, xi = x
            pr, pi = row_of(xr, p), row_of(xi, p)
            qr, qi = row_of(xr, q), row_of(xi, q)
            yr = jnp.where(keep, xr, 0.0) - (fp[0] * pr - fp[1] * pi) - (fq[0] * qr - fq[1] * qi)
            yi = jnp.where(keep, xi, 0.0) - (fp[0] * pi + fp[1] * pr) - (fq[0] * qi + fq[1] * qr)
            return yr, yi

        for t in range(q + 1, ROWS):
            cols[t] = step(cols[t])
        work = [step(x) for x in work]
    head_r, head_i = work[home]
    update, final = list(work), list(work)
    update[home] = (jnp.where(in_block, eye - head_r, head_r), jnp.where(in_block, -head_i, head_i))
    final[home] = (jnp.where(in_block, -head_r, head_r), jnp.where(in_block, -head_i, head_i))
    return update, final


def apply_sweep(panel, update, first):
    home, off = divmod(first, LANES)
    out = list(panel)
    cols = [
        (lane_of(panel[home][0], off + t), lane_of(panel[home][1], off + t)) for t in range(ROWS)
    ]
    for c in range(CHUNKS):
        xr, xi = out[c]
        for t in range(ROWS):
            cr, ci = cols[t]
            ur, ui = row_of(update[c][0], t), row_of(update[c][1], t)
            xr = xr - (cr * ur - ci * ui)
            xi = xi - (cr * ui + ci * ur)
        out[c] = (xr, xi)
    return out


def stack_parts(rows, order):
    parts = split3(jnp.concatenate(rows, axis=0))
    return jnp.concatenate([parts[i] for i in order], axis=0)


LEFT = (0, 0, 0, 1, 1, 2)
RIGHT = (0, 1, 2, 0, 1, 0)


def main_kernel(buf_ref, atom_ref, energy_ref, weight_ref, out_ref, re_ref, im_ref, rows_ref, out_tmp):
    freq = lax.axis_index("freq")
    kpt = lax.axis_index("kpt")
    omega = (2.0 * freq.astype(f32) + 1.0) * math.pi * BETA_INV
    total = (weight_ref[0] + weight_ref[1]).astype(f32)
    own = jnp.where(kpt == 0, weight_ref[0], weight_ref[1]).astype(f32)

    atom = atom_ref[...]
    base = (atom >> 1) * 16 + (atom & 1) * 5
    lane_row = lax.broadcasted_iota(jnp.int32, (1, LANES), 1)
    target = jnp.concatenate([base + o for o in range(ORBS)] + [(lane_row >> 1) * 16 + 10], axis=1)
    pick = (lax.broadcasted_iota(jnp.int32, (1024, 768), 0) == target).astype(f32).astype(bf16)
    turned = lax.dot_general(
        buf_ref[...], pick, (((0,), (0,)), ((), ())), preferred_element_type=f32
    )
    proj_t = [turned[:, LANES * o : LANES * (o + 1)] for o in range(ORBS)]
    sig_parts = turned[0:128, 640:768] + turned[128:256, 640:768] + turned[256:384, 640:768]
    odd = (lax.broadcasted_iota(jnp.int32, (64, LANES), 1) & 1) == 1
    sig = jnp.where(odd, sig_parts[64:128, :], sig_parts[0:64, :])

    proj_b = turned[:, 0:640].astype(bf16)
    for x in range(2):
        for m in range(ORBS):
            acc = None
            for o in range(ORBS):
                i = x * 25 + m * 5 + o
                term = sig[i : i + 1, :] * proj_t[o]
                acc = term if acc is None else acc + term
            rows_ref[x * BANDS : (x + 1) * BANDS, LANES * m : LANES * (m + 1)] = acc.astype(bf16)
    ups = lax.dot_general(
        rows_ref[...], proj_b, (((1,), (1,)), ((), ())), preferred_element_type=f32
    )
    up_r, up_i = ups[0:BANDS, :], ups[BANDS : 2 * BANDS, :]
    ii = lax.broadcasted_iota(jnp.int32, (BANDS, BANDS), 0)
    jj = lax.broadcasted_iota(jnp.int32, (BANDS, BANDS), 1)
    x_mat = jnp.where(ii == jj, -energy_ref[...], 0.0) - 0.5 * (up_r + up_r.T)
    y_mat = jnp.where(ii == jj, omega, 0.0) - 0.5 * (up_i + up_i.T)
    for c in range(CHUNKS):
        re_ref[c, :, :] = x_mat[:, LANES * c : LANES * (c + 1)]
        im_ref[c, :, :] = y_mat[:, LANES * c : LANES * (c + 1)]

    sub_iota = lax.broadcasted_iota(jnp.int32, (ROWS, LANES), 0)
    lane_iota = lax.broadcasted_iota(jnp.int32, (ROWS, LANES), 1)

    def load(first):
        return [(re_ref[c, first : first + ROWS, :], im_ref[c, first : first + ROWS, :]) for c in range(CHUNKS)]

    def masked(panel, firsts):
        out = []
        for c in range(CHUNKS):
            r, i = panel[c]
            for first in firsts:
                home, off = divmod(first, LANES)
                if home == c:
                    gone = (lane_iota >= off) & (lane_iota < off + ROWS)
                    r, i = jnp.where(gone, 0.0, r), jnp.where(gone, 0.0, i)
            out.append((r, i))
        return out

    window = [load(ROWS * g) for g in range(GROUP)]
    for g in range(BANDS // (GROUP * ROWS)):
        firsts = [ROWS * (GROUP * g + n) for n in range(GROUP)]
        last = firsts[-1] + ROWS == BANDS
        ahead = [] if last else [load(first + GROUP * ROWS) for first in firsts]
        lefts, updates = [], []
        for n in range(GROUP):
            first = firsts[n]
            update, final = sweep_panel(window[n], first, sub_iota, lane_iota)
            for c in range(CHUNKS):
                re_ref[c, first : first + ROWS, :] = final[c][0]
                im_ref[c, first : first + ROWS, :] = final[c][1]
            lefts.append(masked(window[n], firsts[n:]))
            updates.append(update)
            for m in range(n + 1, GROUP):
                window[m] = apply_sweep(window[m], update, first)
            ahead = [apply_sweep(panel, update, first) for panel in ahead]
        window = ahead
        left = jnp.concatenate(
            [stack_parts([part for panel in lefts for part in panel[c]], LEFT) for c in range(CHUNKS)],
            axis=1,
        )
        for z in range(CHUNKS):
            rows_re, rows_im = [], []
            for update in updates:
                r, i = update[z]
                rows_re += [r, -i]
                rows_im += [i, r]
            right = jnp.concatenate([stack_parts(rows_re, RIGHT), stack_parts(rows_im, RIGHT)], axis=1)
            prod = lax.dot_general(left, right, (((0,), (0,)), ((), ())), preferred_element_type=f32)
            re_ref[z, :, :] = re_ref[z, :, :] - prod[:, 0:LANES]
            im_ref[z, :, :] = im_ref[z, :, :] - prod[:, LANES:]

    wide = []
    for ref in (re_ref, im_ref):
        full = jnp.concatenate([ref[c, :, :] for c in range(CHUNKS)], axis=1)
        hi = full.astype(bf16)
        low = (full - hi.astype(f32)).astype(bf16)
        wide.append(jnp.concatenate([hi, low], axis=1))
    left = jnp.concatenate(wide, axis=0)
    twice = jnp.concatenate([proj_b, proj_b], axis=0)
    gp = lax.dot_general(left, twice, (((1,), (0,)), ((), ())), preferred_element_type=f32)
    scale = -own / total
    out_tmp[...] = jnp.zeros_like(out_tmp)
    for x in range(2):
        for m in range(ORBS):
            v = gp[x * BANDS : (x + 1) * BANDS, LANES * m : LANES * (m + 1)]
            for o in range(m, ORBS):
                val = jnp.sum(v * proj_t[o], axis=0, keepdims=True) * scale
                i1, i2 = x * 25 + m * 5 + o, x * 25 + o * 5 + m
                out_tmp[i1 : i1 + 1, :] = val
                if o != m:
                    out_tmp[i2 : i2 + 1, :] = val
    out_ref[...] = out_tmp[...].T


def vmem():
    return pl.BlockSpec(memory_space=pltpu.VMEM)


def local(band_energy, projector, sigma, atom_of_slot, kweight):
    packed = pl.pallas_call(
        pack_kernel,
        out_shape=jax.ShapeDtypeStruct((64, 16, BANDS), bf16),
        in_specs=[vmem(), vmem()],
        out_specs=vmem(),
        scratch_shapes=[pltpu.VMEM((LANES, LANES), f32)],
        name="pack",
    )(projector.reshape(10, BANDS), sigma.reshape(PARTS, 2, 64))
    arrived = lax.all_to_all(packed, "freq", split_axis=0, concat_axis=0, tiled=True)
    blocks = pl.pallas_call(
        main_kernel,
        out_shape=jax.ShapeDtypeStruct((ATOMS, LANES), f32),
        in_specs=[vmem(), vmem(), vmem(), pl.BlockSpec(memory_space=pltpu.SMEM)],
        out_specs=vmem(),
        scratch_shapes=[
            pltpu.VMEM((CHUNKS, BANDS, LANES), f32),
            pltpu.VMEM((CHUNKS, BANDS, LANES), f32),
            pltpu.VMEM((2 * BANDS, 640), bf16),
            pltpu.VMEM((LANES, LANES), f32),
        ],
        name="green",
    )(arrived.reshape(1024, BANDS), atom_of_slot.reshape(1, ATOMS), band_energy, kweight)
    back = lax.all_to_all(
        blocks.reshape(ATOMS, 1, LANES), ("freq", "kpt"), split_axis=0, concat_axis=0, tiled=True
    )
    out = pl.pallas_call(
        unpack_kernel,
        out_shape=jax.ShapeDtypeStruct((PARTS, 1, 64), f32),
        in_specs=[vmem()],
        out_specs=vmem(),
        name="unpack",
    )(back.reshape(ATOMS, LANES))
    return out.reshape(2, ORBS, ORBS, 1, 64)


def solution(mesh):
    placed = (P("kpt", None), P("kpt", "freq", None), P(None, None, None, "freq", None), P(), P())
    return jax.shard_map(
        local,
        mesh=mesh,
        in_specs=placed,
        out_specs=P(None, None, None, ("freq", "kpt"), None),
        check_vma=False,
    )
```

```python
import math

import jax
import jax.numpy as jnp
from jax import lax
from jax.experimental import pallas as pl
from jax.experimental.pallas import tpu as pltpu
from jax.sharding import PartitionSpec as P

BANDS = 384
ATOMS = 128
ORBS = 5
PARTS = 2 * ORBS * ORBS
BETA_INV = 0.1
LANES = 128
CHUNKS = BANDS // LANES
ROWS = 8
GROUP = 2

f32 = jnp.float32
bf16 = jnp.bfloat16


def split3(x):
    hi = x.astype(bf16)
    rest = x - hi.astype(f32)
    mid = rest.astype(bf16)
    low = (rest - mid.astype(f32)).astype(bf16)
    return hi, mid, low


def pack_kernel(proj_ref, sig_ref, out_ref, tmp_ref):
    tmp_ref[...] = jnp.zeros_like(tmp_ref)
    tmp_ref[0:PARTS, 0:64] = sig_ref[:, 0, :]
    tmp_ref[64 : 64 + PARTS, 0:64] = sig_ref[:, 1, :]
    turned = tmp_ref[...].T
    hi, mid, low = split3(turned)
    parts = [hi.astype(f32), mid.astype(f32), low.astype(f32)]
    rows = lax.broadcasted_iota(jnp.int32, (16, LANES), 0)
    base = [
        jnp.concatenate(
            [proj_ref[:, LANES * c : LANES * (c + 1)].astype(f32), jnp.zeros((6, LANES), f32)], axis=0
        )
        for c in range(3)
    ]
    for n in range(64):
        for c in range(3):
            row = jnp.broadcast_to(parts[c][n : n + 1, :], (16, LANES))
            out_ref[n, :, LANES * c : LANES * (c + 1)] = jnp.where(rows == 10, row, base[c]).astype(bf16)


def unpack_kernel(in_ref, out_ref):
    both = in_ref[pl.ds(0, 64, stride=2), :] + in_ref[pl.ds(1, 64, stride=2), :]
    turned = both.T
    for i in range(PARTS):
        out_ref[i, :, :] = turned[i : i + 1, :]


def cmul(ar, ai, br, bi):
    return ar * br - ai * bi, ar * bi + ai * br


def row_of(x, i):
    return jnp.broadcast_to(x[i : i + 1, :], (ROWS, LANES))


def lane_of(x, i, zero):
    return jnp.broadcast_to(x[:, i : i + 1], (ROWS, LANES)) + zero


def sweep_panel(panel, first, sub_iota, lane_iota, zero):
    home, off = divmod(first, LANES)
    diag = panel[home]
    cols = [(lane_of(diag[0], off + t, zero), lane_of(diag[1], off + t, zero)) for t in range(ROWS)]
    in_block = (lane_iota >= off) & (lane_iota < off + ROWS)
    eye = jnp.where(lane_iota == sub_iota + off, 1.0, 0.0).astype(f32)
    work = list(panel)
    work[home] = (jnp.where(in_block, eye, diag[0]), jnp.where(in_block, 0.0, diag[1]))
    for p in range(0, ROWS, 2):
        q = p + 1
        ar, ai = row_of(cols[p][0], p), row_of(cols[p][1], p)
        br, bi = row_of(cols[q][0], p), row_of(cols[q][1], p)
        dr, di = row_of(cols[q][0], q), row_of(cols[q][1], q)
        adr, adi = cmul(ar, ai, dr, di)
        bbr, bbi = cmul(br, bi, br, bi)
        det_r, det_i = adr - bbr, adi - bbi
        inv = 1.0 / (det_r * det_r + det_i * det_i)
        vr, vi = det_r * inv, -(det_i * inv)
        w11 = cmul(dr, di, vr, vi)
        w22 = cmul(ar, ai, vr, vi)
        w12 = cmul(-br, -bi, vr, vi)
        cpr, cpi = cols[p]
        cqr, cqi = cols[q]
        t1, t2 = cmul(cpr, cpi, *w11), cmul(cqr, cqi, *w12)
        t3, t4 = cmul(cpr, cpi, *w12), cmul(cqr, cqi, *w22)
        at_p, at_q = sub_iota == p, sub_iota == q
        fp = [jnp.where(at_p, -w11[z], jnp.where(at_q, -w12[z], t1[z] + t2[z])) for z in range(2)]
        fq = [jnp.where(at_p, -w12[z], jnp.where(at_q, -w22[z], t3[z] + t4[z])) for z in range(2)]
        keep = ~(at_p | at_q)

        def step(x):
            xr, xi = x
            pr, pi = row_of(xr, p), row_of(xi, p)
            qr, qi = row_of(xr, q), row_of(xi, q)
            yr = jnp.where(keep, xr, 0.0) - (fp[0] * pr - fp[1] * pi) - (fq[0] * qr - fq[1] * qi)
            yi = jnp.where(keep, xi, 0.0) - (fp[0] * pi + fp[1] * pr) - (fq[0] * qi + fq[1] * qr)
            return yr, yi

        for t in range(q + 1, ROWS):
            cols[t] = step(cols[t])
        work = [step(x) for x in work]
    head_r, head_i = work[home]
    update, final = list(work), list(work)
    update[home] = (jnp.where(in_block, eye - head_r, head_r), jnp.where(in_block, -head_i, head_i))
    final[home] = (jnp.where(in_block, -head_r, head_r), jnp.where(in_block, -head_i, head_i))
    return update, final


def apply_sweep(panel, update, first):
    home, off = divmod(first, LANES)
    out = list(panel)
    cols = [
        tuple(jnp.broadcast_to(part[:, off + t : off + t + 1], (ROWS, LANES)) for part in panel[home])
        for t in range(ROWS)
    ]
    for c in range(CHUNKS):
        xr, xi = out[c]
        for t in range(ROWS):
            cr, ci = cols[t]
            ur, ui = row_of(update[c][0], t), row_of(update[c][1], t)
            xr = xr - (cr * ur - ci * ui)
            xi = xi - (cr * ui + ci * ur)
        out[c] = (xr, xi)
    return out


def stack_parts(rows, order):
    parts = split3(jnp.concatenate(rows, axis=0))
    return jnp.concatenate([parts[i] for i in order], axis=0)


LEFT = (0, 0, 0, 1, 1, 2)
RIGHT = (0, 1, 2, 0, 1, 0)


def main_kernel(buf_ref, atom_ref, energy_ref, weight_ref, out_ref, re_ref, im_ref, rows_ref, out_tmp):
    freq = lax.axis_index("freq")
    kpt = lax.axis_index("kpt")
    omega = (2.0 * freq.astype(f32) + 1.0) * math.pi * BETA_INV
    total = (weight_ref[0] + weight_ref[1]).astype(f32)
    own = jnp.where(kpt == 0, weight_ref[0], weight_ref[1]).astype(f32)

    atom = atom_ref[...]
    base = (atom >> 1) * 16 + (atom & 1) * 5
    lane_row = lax.broadcasted_iota(jnp.int32, (1, LANES), 1)
    target = jnp.concatenate([base + o for o in range(ORBS)] + [(lane_row >> 1) * 16 + 10], axis=1)
    pick = (lax.broadcasted_iota(jnp.int32, (1024, 768), 0) == target).astype(f32).astype(bf16)
    turned = lax.dot_general(
        buf_ref[...], pick, (((0,), (0,)), ((), ())), preferred_element_type=f32
    )
    proj_t = [turned[:, LANES * o : LANES * (o + 1)] for o in range(ORBS)]
    sig_parts = turned[0:128, 640:768] + turned[128:256, 640:768] + turned[256:384, 640:768]
    odd = (lax.broadcasted_iota(jnp.int32, (64, LANES), 1) & 1) == 1
    sig = jnp.where(odd, sig_parts[64:128, :], sig_parts[0:64, :])

    proj_b = turned[:, 0:640].astype(bf16)
    for x in range(2):
        for m in range(ORBS):
            acc = None
            for o in range(ORBS):
                i = x * 25 + m * 5 + o
                term = sig[i : i + 1, :] * proj_t[o]
                acc = term if acc is None else acc + term
            rows_ref[x * BANDS : (x + 1) * BANDS, LANES * m : LANES * (m + 1)] = acc.astype(bf16)
    ups = lax.dot_general(
        rows_ref[...], proj_b, (((1,), (1,)), ((), ())), preferred_element_type=f32
    )
    up_r, up_i = ups[0:BANDS, :], ups[BANDS : 2 * BANDS, :]
    ii = lax.broadcasted_iota(jnp.int32, (BANDS, BANDS), 0)
    jj = lax.broadcasted_iota(jnp.int32, (BANDS, BANDS), 1)
    x_mat = jnp.where(ii == jj, -energy_ref[...], 0.0) - 0.5 * (up_r + up_r.T)
    y_mat = jnp.where(ii == jj, omega, 0.0) - 0.5 * (up_i + up_i.T)
    for c in range(CHUNKS):
        re_ref[c, :, :] = x_mat[:, LANES * c : LANES * (c + 1)]
        im_ref[c, :, :] = y_mat[:, LANES * c : LANES * (c + 1)]

    sub_iota = lax.broadcasted_iota(jnp.int32, (ROWS, LANES), 0)
    lane_iota = lax.broadcasted_iota(jnp.int32, (ROWS, LANES), 1)
    zero = jnp.broadcast_to(energy_ref[:, 0:LANES] * 0.0, (ROWS, LANES))

    def load(first):
        return [(re_ref[c, first : first + ROWS, :], im_ref[c, first : first + ROWS, :]) for c in range(CHUNKS)]

    def masked(panel, firsts):
        out = []
        for c in range(CHUNKS):
            r, i = panel[c]
            for first in firsts:
                home, off = divmod(first, LANES)
                if home == c:
                    gone = (lane_iota >= off) & (lane_iota < off + ROWS)
                    r, i = jnp.where(gone, 0.0, r), jnp.where(gone, 0.0, i)
            out.append((r, i))
        return out

    window = [load(ROWS * g) for g in range(GROUP)]
    for g in range(BANDS // (GROUP * ROWS)):
        firsts = [ROWS * (GROUP * g + n) for n in range(GROUP)]
        last = firsts[-1] + ROWS == BANDS
        ahead = [] if last else [load(first + GROUP * ROWS) for first in firsts]
        lefts, updates = [], []
        for n in range(GROUP):
            first = firsts[n]
            update, final = sweep_panel(window[n], first, sub_iota, lane_iota, zero)
            for c in range(CHUNKS):
                re_ref[c, first : first + ROWS, :] = final[c][0]
                im_ref[c, first : first + ROWS, :] = final[c][1]
            lefts.append(masked(window[n], firsts[n:]))
            updates.append(update)
            for m in range(n + 1, GROUP):
                window[m] = apply_sweep(window[m], update, first)
            ahead = [apply_sweep(panel, update, first) for panel in ahead]
        window = ahead
        left = jnp.concatenate(
            [stack_parts([part for panel in lefts for part in panel[c]], LEFT) for c in range(CHUNKS)],
            axis=1,
        )
        for z in range(CHUNKS):
            rows_re, rows_im = [], []
            for update in updates:
                r, i = update[z]
                rows_re += [r, -i]
                rows_im += [i, r]
            right = jnp.concatenate([stack_parts(rows_re, RIGHT), stack_parts(rows_im, RIGHT)], axis=1)
            prod = lax.dot_general(left, right, (((0,), (0,)), ((), ())), preferred_element_type=f32)
            re_ref[z, :, :] = re_ref[z, :, :] - prod[:, 0:LANES]
            im_ref[z, :, :] = im_ref[z, :, :] - prod[:, LANES:]

    wide = []
    for ref in (re_ref, im_ref):
        full = jnp.concatenate([ref[c, :, :] for c in range(CHUNKS)], axis=1)
        hi = full.astype(bf16)
        low = (full - hi.astype(f32)).astype(bf16)
        wide.append(jnp.concatenate([hi, low], axis=1))
    left = jnp.concatenate(wide, axis=0)
    twice = jnp.concatenate([proj_b, proj_b], axis=0)
    gp = lax.dot_general(left, twice, (((1,), (0,)), ((), ())), preferred_element_type=f32)
    scale = -own / total
    out_tmp[...] = jnp.zeros_like(out_tmp)
    for x in range(2):
        for m in range(ORBS):
            v = gp[x * BANDS : (x + 1) * BANDS, LANES * m : LANES * (m + 1)]
            for o in range(m, ORBS):
                val = jnp.sum(v * proj_t[o], axis=0, keepdims=True) * scale
                i1, i2 = x * 25 + m * 5 + o, x * 25 + o * 5 + m
                out_tmp[i1 : i1 + 1, :] = val
                if o != m:
                    out_tmp[i2 : i2 + 1, :] = val
    out_ref[...] = out_tmp[...].T


def vmem():
    return pl.BlockSpec(memory_space=pltpu.VMEM)


def local(band_energy, projector, sigma, atom_of_slot, kweight):
    packed = pl.pallas_call(
        pack_kernel,
        out_shape=jax.ShapeDtypeStruct((64, 16, BANDS), bf16),
        in_specs=[vmem(), vmem()],
        out_specs=vmem(),
        scratch_shapes=[pltpu.VMEM((LANES, LANES), f32)],
        compiler_params=pltpu.CompilerParams(vmem_limit_bytes=8 * 2**20),
        name="pack",
    )(projector.reshape(10, BANDS), sigma.reshape(PARTS, 2, 64))
    arrived = lax.all_to_all(packed, "freq", split_axis=0, concat_axis=0, tiled=True)
    blocks = pl.pallas_call(
        main_kernel,
        out_shape=jax.ShapeDtypeStruct((ATOMS, LANES), f32),
        in_specs=[vmem(), vmem(), vmem(), pl.BlockSpec(memory_space=pltpu.SMEM)],
        out_specs=vmem(),
        scratch_shapes=[
            pltpu.VMEM((CHUNKS, BANDS, LANES), f32),
            pltpu.VMEM((CHUNKS, BANDS, LANES), f32),
            pltpu.VMEM((2 * BANDS, 640), bf16),
            pltpu.VMEM((LANES, LANES), f32),
        ],
        compiler_params=pltpu.CompilerParams(vmem_limit_bytes=24 * 2**20),
        name="green",
    )(arrived.reshape(1024, BANDS), atom_of_slot.reshape(1, ATOMS), band_energy, kweight)
    back = lax.all_to_all(
        blocks.reshape(ATOMS, 1, LANES), ("freq", "kpt"), split_axis=0, concat_axis=0, tiled=True
    )
    out = pl.pallas_call(
        unpack_kernel,
        out_shape=jax.ShapeDtypeStruct((PARTS, 1, 64), f32),
        in_specs=[vmem()],
        out_specs=vmem(),
        compiler_params=pltpu.CompilerParams(vmem_limit_bytes=8 * 2**20),
        name="unpack",
    )(back.reshape(ATOMS, LANES))
    return out.reshape(2, ORBS, ORBS, 1, 64)


def solution(mesh):
    placed = (P("kpt", None), P("kpt", "freq", None), P(None, None, None, "freq", None), P(), P())
    return jax.shard_map(
        local,
        mesh=mesh,
        in_specs=placed,
        out_specs=P(None, None, None, ("freq", "kpt"), None),
        check_vma=False,
    )
```

```python
import math

import jax
import jax.numpy as jnp
from jax import lax
from jax.experimental import pallas as pl
from jax.experimental.pallas import tpu as pltpu
from jax.sharding import PartitionSpec as P

BANDS = 384
ATOMS = 128
ORBS = 5
PARTS = 2 * ORBS * ORBS
BETA_INV = 0.1
LANES = 128
CHUNKS = BANDS // LANES
ROWS = 8
GROUP = 2
PAIRS = 15

f32 = jnp.float32
bf16 = jnp.bfloat16


def split3(x):
    hi = x.astype(bf16)
    rest = x - hi.astype(f32)
    mid = rest.astype(bf16)
    low = (rest - mid.astype(f32)).astype(bf16)
    return hi, mid, low


def pack_kernel(proj_ref, sig_ref, out_ref, tmp_ref):
    tmp_ref[...] = jnp.zeros_like(tmp_ref)
    tmp_ref[0:PARTS, 0:64] = sig_ref[:, 0, :]
    tmp_ref[64 : 64 + PARTS, 0:64] = sig_ref[:, 1, :]
    turned = tmp_ref[...].T
    hi, mid, low = split3(turned)
    parts = [hi.astype(f32), mid.astype(f32), low.astype(f32)]
    rows = lax.broadcasted_iota(jnp.int32, (16, LANES), 0)
    base = [
        jnp.concatenate(
            [proj_ref[:, LANES * c : LANES * (c + 1)].astype(f32), jnp.zeros((6, LANES), f32)], axis=0
        )
        for c in range(3)
    ]
    for n in range(64):
        for c in range(3):
            row = jnp.broadcast_to(parts[c][n : n + 1, :], (16, LANES))
            out_ref[n, :, LANES * c : LANES * (c + 1)] = jnp.where(rows == 10, row, base[c]).astype(bf16)


def unpack_kernel(in_ref, out_ref):
    both = in_ref[pl.ds(0, 64, stride=2), :] + in_ref[pl.ds(1, 64, stride=2), :]
    turned = both.T
    for i in range(PARTS):
        out_ref[i, :, :] = turned[i : i + 1, :]


def cmul(ar, ai, br, bi):
    return ar * br - ai * bi, ar * bi + ai * br


def row_of(x, i):
    return jnp.broadcast_to(x[i : i + 1, :], (ROWS, LANES))


def lane_of(x, i, zero):
    return jnp.broadcast_to(x[:, i : i + 1], (ROWS, LANES)) + zero


def sweep_panel(panel, off, sub_iota, lane_iota, zero):
    cols = [(lane_of(panel[0], off + t, zero), lane_of(panel[1], off + t, zero)) for t in range(ROWS)]
    in_block = (lane_iota >= off) & (lane_iota < off + ROWS)
    eye = jnp.where(lane_iota == sub_iota + off, 1.0, 0.0).astype(f32)
    work = (jnp.where(in_block, eye, panel[0]), jnp.where(in_block, 0.0, panel[1]))
    for p in range(0, ROWS, 2):
        q = p + 1
        ar, ai = row_of(cols[p][0], p), row_of(cols[p][1], p)
        br, bi = row_of(cols[q][0], p), row_of(cols[q][1], p)
        dr, di = row_of(cols[q][0], q), row_of(cols[q][1], q)
        adr, adi = cmul(ar, ai, dr, di)
        bbr, bbi = cmul(br, bi, br, bi)
        det_r, det_i = adr - bbr, adi - bbi
        inv = 1.0 / (det_r * det_r + det_i * det_i)
        vr, vi = det_r * inv, -(det_i * inv)
        w11 = cmul(dr, di, vr, vi)
        w22 = cmul(ar, ai, vr, vi)
        w12 = cmul(-br, -bi, vr, vi)
        cpr, cpi = cols[p]
        cqr, cqi = cols[q]
        t1, t2 = cmul(cpr, cpi, *w11), cmul(cqr, cqi, *w12)
        t3, t4 = cmul(cpr, cpi, *w12), cmul(cqr, cqi, *w22)
        at_p, at_q = sub_iota == p, sub_iota == q
        fp = [jnp.where(at_p, -w11[z], jnp.where(at_q, -w12[z], t1[z] + t2[z])) for z in range(2)]
        fq = [jnp.where(at_p, -w12[z], jnp.where(at_q, -w22[z], t3[z] + t4[z])) for z in range(2)]
        keep = ~(at_p | at_q)

        def step(x):
            xr, xi = x
            pr, pi = row_of(xr, p), row_of(xi, p)
            qr, qi = row_of(xr, q), row_of(xi, q)
            yr = jnp.where(keep, xr, 0.0) - (fp[0] * pr - fp[1] * pi) - (fq[0] * qr - fq[1] * qi)
            yi = jnp.where(keep, xi, 0.0) - (fp[0] * pi + fp[1] * pr) - (fq[0] * qi + fq[1] * qr)
            return yr, yi

        for t in range(q + 1, ROWS):
            cols[t] = step(cols[t])
        work = step(work)
    re, im = work
    update = (jnp.where(in_block, eye - re, re), jnp.where(in_block, -im, im))
    final = (jnp.where(in_block, -re, re), jnp.where(in_block, -im, im))
    return update, final


def apply_sweep(panel, update, off):
    xr, xi = panel
    sum_r, sum_i = [], []
    for t in range(ROWS):
        cr = jnp.broadcast_to(panel[0][:, off + t : off + t + 1], (ROWS, LANES))
        ci = jnp.broadcast_to(panel[1][:, off + t : off + t + 1], (ROWS, LANES))
        ur, ui = row_of(update[0], t), row_of(update[1], t)
        pr, pi = cmul(cr, ci, ur, ui)
        sum_r.append(pr)
        sum_i.append(pi)
    return xr - tree(sum_r), xi - tree(sum_i)


def tree(terms):
    while len(terms) > 1:
        terms = [sum(terms[i : i + 2][1:], terms[i]) for i in range(0, len(terms), 2)]
    return terms[0]


LEFT = (0, 0, 1)
RIGHT = (0, 1, 0)


def cat(parts, axis):
    return jnp.concatenate(parts, axis=axis)


def dot(a, b):
    return jnp.dot(a, b, preferred_element_type=f32)


def stack_parts(rows, order):
    parts = split3(cat(rows, 0))
    return cat([parts[i] for i in order], 0)


def mul_wide(a, b):
    ar, ai = split3(a[0]), split3(a[1])
    br, bi, bn = split3(b[0]), split3(b[1]), split3(-b[1])
    left = cat([x for i in LEFT for x in (ar[i], ai[i])], 1)
    right = cat([cat([cat([br[i], bi[i]], 1), cat([bn[i], br[i]], 1)], 0) for i in RIGHT], 0)
    out = dot(left, right)
    n = b[0].shape[1]
    return out[:, 0:n], out[:, n:]


def mul_tall(a, b):
    ar, ai, an = split3(a[0]), split3(a[1]), split3(-a[1])
    br, bi = split3(b[0]), split3(b[1])
    left = cat([cat([cat([ar[i], an[i]], 1), cat([ai[i], ar[i]], 1)], 0) for i in LEFT], 1)
    right = cat([x for i in RIGHT for x in (br[i], bi[i])], 0)
    out = dot(left, right)
    m = a[0].shape[0]
    return out[0:m, :], out[m:, :]


def mul_real(a, exact):
    left = cat(split3(cat([a[0], a[1]], 0)), 1)
    out = dot(left, cat([exact] * 3, 0))
    m = a[0].shape[0]
    return out[0:m, :], out[m:, :]


def add(x, y):
    return x[0] + y[0], x[1] + y[1]


def sweep_block(re_ref, im_ref, k, sub_iota, lane_iota, zero):
    def load(off):
        return re_ref[k, off : off + ROWS, :], im_ref[k, off : off + ROWS, :]

    def masked(panel, off, stop):
        gone = (lane_iota >= off) & (lane_iota < stop)
        return jnp.where(gone, 0.0, panel[0]), jnp.where(gone, 0.0, panel[1])

    span = GROUP * ROWS
    window = [load(ROWS * n) for n in range(GROUP)]
    for base in range(0, LANES, span):
        follow = base + span
        ahead = load(follow) if follow < LANES else None
        lefts, updates = [], []
        for n in range(GROUP):
            off = base + ROWS * n
            update, final = sweep_panel(window[n], off, sub_iota, lane_iota, zero)
            re_ref[k, off : off + ROWS, :] = final[0]
            im_ref[k, off : off + ROWS, :] = final[1]
            lefts.append(masked(window[n], off, follow))
            updates.append(update)
            for m in range(n + 1, GROUP):
                window[m] = apply_sweep(window[m], update, off)
            if ahead is not None:
                ahead = apply_sweep(ahead, update, off)
        left = stack_parts([x for panel in lefts for x in panel], LEFT).T
        right = cat(
            [
                stack_parts([x for r, i in updates for x in (r, -i)], RIGHT),
                stack_parts([x for r, i in updates for x in (i, r)], RIGHT),
            ],
            1,
        )
        if ahead is not None:
            early = dot(left[follow : follow + span, :], right)
            window = [ahead]
            for n in range(1, GROUP):
                at = slice(ROWS * n, ROWS * (n + 1))
                r, i = load(follow + ROWS * n)
                window.append((r - early[at, 0:LANES], i - early[at, LANES:]))
        prod = dot(left, right)
        re_ref[k, :, :] = re_ref[k, :, :] - prod[:, 0:LANES]
        im_ref[k, :, :] = im_ref[k, :, :] - prod[:, LANES:]


def main_kernel(buf_ref, atom_ref, energy_ref, weight_ref, out_ref, re_ref, im_ref, pt_ref, rows_ref, acc_ref, out_tmp):
    freq = lax.axis_index("freq")
    kpt = lax.axis_index("kpt")
    omega = (2.0 * freq.astype(f32) + 1.0) * math.pi * BETA_INV
    total = (weight_ref[0] + weight_ref[1]).astype(f32)
    own = jnp.where(kpt == 0, weight_ref[0], weight_ref[1]).astype(f32)

    atom = atom_ref[...]
    base = (atom >> 1) * 16 + (atom & 1) * 5
    lane_row = lax.broadcasted_iota(jnp.int32, (1, LANES), 1)
    target = jnp.concatenate([base + o for o in range(ORBS)] + [(lane_row >> 1) * 16 + 10], axis=1)
    pick = (lax.broadcasted_iota(jnp.int32, (1024, 768), 0) == target).astype(f32).astype(bf16)
    turned = lax.dot_general(
        buf_ref[...], pick, (((0,), (0,)), ((), ())), preferred_element_type=f32
    )
    proj_t = [turned[:, LANES * o : LANES * (o + 1)] for o in range(ORBS)]
    sig_parts = turned[0:128, 640:768] + turned[128:256, 640:768] + turned[256:384, 640:768]
    odd = (lax.broadcasted_iota(jnp.int32, (64, LANES), 1) & 1) == 1
    sig = jnp.where(odd, sig_parts[64:128, :], sig_parts[0:64, :])

    pt_ref[...] = turned[:, 0:640].astype(bf16)
    proj_b = pt_ref[...]
    for x in range(2):
        for m in range(ORBS):
            acc = None
            for o in range(ORBS):
                i = x * 25 + m * 5 + o
                term = sig[i : i + 1, :] * proj_t[o]
                acc = term if acc is None else acc + term
            rows_ref[x * BANDS : (x + 1) * BANDS, LANES * m : LANES * (m + 1)] = acc.astype(bf16)
    ups = lax.dot_general(
        rows_ref[...], proj_b, (((1,), (1,)), ((), ())), preferred_element_type=f32
    )
    up_r, up_i = ups[0:BANDS, :], ups[BANDS : 2 * BANDS, :]
    ii = lax.broadcasted_iota(jnp.int32, (BANDS, BANDS), 0)
    jj = lax.broadcasted_iota(jnp.int32, (BANDS, BANDS), 1)
    x_mat = jnp.where(ii == jj, -energy_ref[...], 0.0) - 0.5 * (up_r + up_r.T)
    y_mat = jnp.where(ii == jj, omega, 0.0) - 0.5 * (up_i + up_i.T)

    def block(i, j):
        at = (slice(LANES * i, LANES * (i + 1)), slice(LANES * j, LANES * (j + 1)))
        return x_mat[at], y_mat[at]

    sub_iota = lax.broadcasted_iota(jnp.int32, (ROWS, LANES), 0)
    lane_iota = lax.broadcasted_iota(jnp.int32, (ROWS, LANES), 1)
    zero = jnp.broadcast_to(energy_ref[:, 0:LANES] * 0.0, (ROWS, LANES))

    blocks = {(i, j): block(i, j) for i in range(CHUNKS) for j in range(CHUNKS)}
    exact = pt_ref[0:LANES, :]
    for k in range(CHUNKS):
        re_ref[k, :, :], im_ref[k, :, :] = blocks[k, k]
        sweep_block(re_ref, im_ref, k, sub_iota, lane_iota, zero)
        swept = re_ref[k, :, :], im_ref[k, :, :]
        after = range(k + 1, CHUNKS)
        stack = [swept]
        if k + 1 < CHUNKS:
            below = tuple(cat([blocks[i, k][x] for i in after], 0) for x in range(2))
            low = mul_wide(below, swept)
            for j in after:
                change = mul_wide(low, blocks[k, j])
                for i in after:
                    at = slice(LANES * (i - k - 1), LANES * (i - k))
                    blocks[i, j] = add(blocks[i, j], (change[0][at, :], change[1][at, :]))
            stack.append(low)
        lhs = tuple(cat([part[x] for part in stack], 0) for x in range(2))
        wide = mul_real(lhs, exact) if k == 0 else mul_tall(lhs, y[k])
        z = wide[0][0:LANES, :], wide[1][0:LANES, :]
        if k == 0:
            y = [[pt_ref[LANES * i : LANES * (i + 1), :].astype(f32), None] for i in range(CHUNKS)]
        for i in after:
            at = slice(LANES * (i - k), LANES * (i - k + 1))
            y[i] = [y[i][0] + wide[0][at, :], wide[1][at, :] if y[i][1] is None else y[i][1] + wide[1][at, :]]
        n = 0
        for m in range(ORBS):
            for o in range(m, ORBS):
                lm, lo = slice(LANES * m, LANES * (m + 1)), slice(LANES * o, LANES * (o + 1))
                re, im = y[k][0][:, lm] * z[0][:, lo], y[k][0][:, lm] * z[1][:, lo]
                if y[k][1] is not None:
                    re = re - y[k][1][:, lm] * z[1][:, lo]
                    im = im + y[k][1][:, lm] * z[0][:, lo]
                for x, val in ((0, re), (1, im)):
                    val = tree([val[ROWS * r : ROWS * (r + 1), :] for r in range(LANES // ROWS)])
                    at = slice(ROWS * (x * PAIRS + n), ROWS * (x * PAIRS + n + 1))
                    acc_ref[at, :] = val if k == 0 else acc_ref[at, :] + val
                n += 1
    scale = -own / total
    out_tmp[...] = jnp.zeros_like(out_tmp)
    for x in range(2):
        n = 0
        for m in range(ORBS):
            for o in range(m, ORBS):
                at = slice(ROWS * (x * PAIRS + n), ROWS * (x * PAIRS + n + 1))
                val = jnp.sum(acc_ref[at, :], axis=0, keepdims=True) * scale
                n += 1
                for i in {x * 25 + m * 5 + o, x * 25 + o * 5 + m}:
                    out_tmp[i : i + 1, :] = val
    out_ref[...] = out_tmp[...].T


def vmem():
    return pl.BlockSpec(memory_space=pltpu.VMEM)


def local(band_energy, projector, sigma, atom_of_slot, kweight):
    packed = pl.pallas_call(
        pack_kernel,
        out_shape=jax.ShapeDtypeStruct((64, 16, BANDS), bf16),
        in_specs=[vmem(), vmem()],
        out_specs=vmem(),
        scratch_shapes=[pltpu.VMEM((LANES, LANES), f32)],
        compiler_params=pltpu.CompilerParams(vmem_limit_bytes=8 * 2**20),
        name="pack",
    )(projector.reshape(10, BANDS), sigma.reshape(PARTS, 2, 64))
    arrived = lax.all_to_all(packed, "freq", split_axis=0, concat_axis=0, tiled=True)
    blocks = pl.pallas_call(
        main_kernel,
        out_shape=jax.ShapeDtypeStruct((ATOMS, LANES), f32),
        in_specs=[vmem(), vmem(), vmem(), pl.BlockSpec(memory_space=pltpu.SMEM)],
        out_specs=vmem(),
        scratch_shapes=[
            pltpu.VMEM((CHUNKS, LANES, LANES), f32),
            pltpu.VMEM((CHUNKS, LANES, LANES), f32),
            pltpu.VMEM((BANDS, 640), bf16),
            pltpu.VMEM((2 * BANDS, 640), bf16),
            pltpu.VMEM((2 * PAIRS * ROWS, LANES), f32),
            pltpu.VMEM((LANES, LANES), f32),
        ],
        compiler_params=pltpu.CompilerParams(vmem_limit_bytes=24 * 2**20),
        name="green",
    )(arrived.reshape(1024, BANDS), atom_of_slot.reshape(1, ATOMS), band_energy, kweight)
    back = lax.all_to_all(
        blocks.reshape(ATOMS, 1, LANES), ("freq", "kpt"), split_axis=0, concat_axis=0, tiled=True
    )
    out = pl.pallas_call(
        unpack_kernel,
        out_shape=jax.ShapeDtypeStruct((PARTS, 1, 64), f32),
        in_specs=[vmem()],
        out_specs=vmem(),
        compiler_params=pltpu.CompilerParams(vmem_limit_bytes=8 * 2**20),
        name="unpack",
    )(back.reshape(ATOMS, LANES))
    return out.reshape(2, ORBS, ORBS, 1, 64)


def solution(mesh):
    placed = (P("kpt", None), P("kpt", "freq", None), P(None, None, None, "freq", None), P(), P())
    return jax.shard_map(
        local,
        mesh=mesh,
        in_specs=placed,
        out_specs=P(None, None, None, ("freq", "kpt"), None),
        check_vma=False,
    )
```

```python
import math

import jax
import jax.numpy as jnp
from jax import lax
from jax.experimental import pallas as pl
from jax.experimental.pallas import tpu as pltpu
from jax.sharding import PartitionSpec as P

BANDS = 384
ATOMS = 128
ORBS = 5
PARTS = 2 * ORBS * ORBS
BETA_INV = 0.1
LANES = 128
CHUNKS = BANDS // LANES
ROWS = 8
GROUP = 2
PAIRS = 15

f32 = jnp.float32
bf16 = jnp.bfloat16


def split3(x):
    hi = x.astype(bf16)
    rest = x - hi.astype(f32)
    mid = rest.astype(bf16)
    low = (rest - mid.astype(f32)).astype(bf16)
    return hi, mid, low


def pack_kernel(
    proj_hbm, sig_hbm, atom_hbm, energy_hbm, weight_hbm,
    out_ref, atom_ref, energy_ref, scale_ref,
    proj_ref, sig_ref, weight_ref, tmp_ref, sems,
):
    pairs = (
        (sig_hbm, sig_ref), (proj_hbm, proj_ref), (atom_hbm, atom_ref),
        (energy_hbm, energy_ref), (weight_hbm, weight_ref),
    )
    copies = [pltpu.make_async_copy(src, dst, sems.at[i]) for i, (src, dst) in enumerate(pairs)]
    for copy in copies:
        copy.start()
    for copy in copies:
        copy.wait()
    total = (weight_ref[0] + weight_ref[1]).astype(f32)
    own = jnp.where(lax.axis_index("kpt") == 0, weight_ref[0], weight_ref[1]).astype(f32)
    scale_ref[...] = jnp.full((1, LANES), -own, f32) / jnp.full((1, LANES), total, f32)
    tmp_ref[...] = jnp.zeros_like(tmp_ref)
    tmp_ref[0:PARTS, 0:64] = sig_ref[:, 0, :]
    tmp_ref[64 : 64 + PARTS, 0:64] = sig_ref[:, 1, :]
    turned = tmp_ref[...].T
    hi, mid, low = split3(turned)
    parts = [hi.astype(f32), mid.astype(f32), low.astype(f32)]
    rows = lax.broadcasted_iota(jnp.int32, (16, LANES), 0)
    base = [
        jnp.concatenate(
            [proj_ref[:, LANES * c : LANES * (c + 1)].astype(f32), jnp.zeros((6, LANES), f32)], axis=0
        )
        for c in range(3)
    ]
    for n in range(64):
        for c in range(3):
            row = jnp.broadcast_to(parts[c][n : n + 1, :], (16, LANES))
            out_ref[n, :, LANES * c : LANES * (c + 1)] = jnp.where(rows == 10, row, base[c]).astype(bf16)


def unpack_kernel(in_ref, out_ref):
    both = in_ref[pl.ds(0, 64, stride=2), :] + in_ref[pl.ds(1, 64, stride=2), :]
    turned = both.T
    for i in range(PARTS):
        out_ref[i, :, :] = turned[i : i + 1, :]


def cmul(ar, ai, br, bi):
    return ar * br - ai * bi, ar * bi + ai * br


def row_of(x, i):
    return jnp.broadcast_to(x[i : i + 1, :], (ROWS, LANES))


def lane_of(x, i, zero):
    return jnp.broadcast_to(x[:, i : i + 1], (ROWS, LANES)) + zero


def sweep_panel(panel, off, sub_iota, lane_iota, zero):
    cols = [(lane_of(panel[0], off + t, zero), lane_of(panel[1], off + t, zero)) for t in range(ROWS)]
    in_block = (lane_iota >= off) & (lane_iota < off + ROWS)
    eye = jnp.where(lane_iota == sub_iota + off, 1.0, 0.0).astype(f32)
    work = (jnp.where(in_block, eye, panel[0]), jnp.where(in_block, 0.0, panel[1]))
    for p in range(0, ROWS, 2):
        q = p + 1
        ar, ai = row_of(cols[p][0], p), row_of(cols[p][1], p)
        br, bi = row_of(cols[q][0], p), row_of(cols[q][1], p)
        dr, di = row_of(cols[q][0], q), row_of(cols[q][1], q)
        adr, adi = cmul(ar, ai, dr, di)
        bbr, bbi = cmul(br, bi, br, bi)
        det_r, det_i = adr - bbr, adi - bbi
        inv = 1.0 / (det_r * det_r + det_i * det_i)
        vr, vi = det_r * inv, -(det_i * inv)
        w11 = cmul(dr, di, vr, vi)
        w22 = cmul(ar, ai, vr, vi)
        w12 = cmul(-br, -bi, vr, vi)
        cpr, cpi = cols[p]
        cqr, cqi = cols[q]
        t1, t2 = cmul(cpr, cpi, *w11), cmul(cqr, cqi, *w12)
        t3, t4 = cmul(cpr, cpi, *w12), cmul(cqr, cqi, *w22)
        at_p, at_q = sub_iota == p, sub_iota == q
        fp = [jnp.where(at_p, -w11[z], jnp.where(at_q, -w12[z], t1[z] + t2[z])) for z in range(2)]
        fq = [jnp.where(at_p, -w12[z], jnp.where(at_q, -w22[z], t3[z] + t4[z])) for z in range(2)]
        keep = ~(at_p | at_q)

        def step(x):
            xr, xi = x
            pr, pi = row_of(xr, p), row_of(xi, p)
            qr, qi = row_of(xr, q), row_of(xi, q)
            yr = jnp.where(keep, xr, 0.0) - (fp[0] * pr - fp[1] * pi) - (fq[0] * qr - fq[1] * qi)
            yi = jnp.where(keep, xi, 0.0) - (fp[0] * pi + fp[1] * pr) - (fq[0] * qi + fq[1] * qr)
            return yr, yi

        for t in range(q + 1, ROWS):
            cols[t] = step(cols[t])
        work = step(work)
    re, im = work
    update = (jnp.where(in_block, eye - re, re), jnp.where(in_block, -im, im))
    final = (jnp.where(in_block, -re, re), jnp.where(in_block, -im, im))
    return update, final


def apply_sweep(panel, update, off):
    xr, xi = panel
    sum_r, sum_i = [], []
    for t in range(ROWS):
        cr = jnp.broadcast_to(panel[0][:, off + t : off + t + 1], (ROWS, LANES))
        ci = jnp.broadcast_to(panel[1][:, off + t : off + t + 1], (ROWS, LANES))
        ur, ui = row_of(update[0], t), row_of(update[1], t)
        pr, pi = cmul(cr, ci, ur, ui)
        sum_r.append(pr)
        sum_i.append(pi)
    return xr - tree(sum_r), xi - tree(sum_i)


def tree(terms):
    while len(terms) > 1:
        terms = [sum(terms[i : i + 2][1:], terms[i]) for i in range(0, len(terms), 2)]
    return terms[0]


LEFT = (0, 0, 1)
RIGHT = (0, 1, 0)


def cat(parts, axis):
    return jnp.concatenate(parts, axis=axis)


def dot(a, b):
    return jnp.dot(a, b, preferred_element_type=f32)


def stack_parts(rows, order):
    parts = split3(cat(rows, 0))
    return cat([parts[i] for i in order], 0)


def mul_wide(a, b):
    ar, ai = split3(a[0]), split3(a[1])
    br, bi, bn = split3(b[0]), split3(b[1]), split3(-b[1])
    left = cat([x for i in LEFT for x in (ar[i], ai[i])], 1)
    right = cat([cat([cat([br[i], bi[i]], 1), cat([bn[i], br[i]], 1)], 0) for i in RIGHT], 0)
    out = dot(left, right)
    n = b[0].shape[1]
    return out[:, 0:n], out[:, n:]


def mul_tall(a, b):
    ar, ai, an = split3(a[0]), split3(a[1]), split3(-a[1])
    br, bi = split3(b[0]), split3(b[1])
    left = cat([cat([cat([ar[i], an[i]], 1), cat([ai[i], ar[i]], 1)], 0) for i in LEFT], 1)
    right = cat([x for i in RIGHT for x in (br[i], bi[i])], 0)
    out = dot(left, right)
    m = a[0].shape[0]
    return out[0:m, :], out[m:, :]


def mul_real(a, exact):
    left = cat(split3(cat([a[0], a[1]], 0)), 1)
    out = dot(left, cat([exact] * 3, 0))
    m = a[0].shape[0]
    return out[0:m, :], out[m:, :]


def add(x, y):
    return x[0] + y[0], x[1] + y[1]


def sweep_block(re_ref, im_ref, k, sub_iota, lane_iota, zero):
    def load(off):
        return re_ref[k, off : off + ROWS, :], im_ref[k, off : off + ROWS, :]

    def masked(panel, off, stop):
        gone = (lane_iota >= off) & (lane_iota < stop)
        return jnp.where(gone, 0.0, panel[0]), jnp.where(gone, 0.0, panel[1])

    span = GROUP * ROWS
    window = [load(ROWS * n) for n in range(GROUP)]
    for base in range(0, LANES, span):
        follow = base + span
        ahead = load(follow) if follow < LANES else None
        lefts, updates = [], []
        for n in range(GROUP):
            off = base + ROWS * n
            update, final = sweep_panel(window[n], off, sub_iota, lane_iota, zero)
            re_ref[k, off : off + ROWS, :] = final[0]
            im_ref[k, off : off + ROWS, :] = final[1]
            lefts.append(masked(window[n], off, follow))
            updates.append(update)
            for m in range(n + 1, GROUP):
                window[m] = apply_sweep(window[m], update, off)
            if ahead is not None:
                ahead = apply_sweep(ahead, update, off)
        left = stack_parts([x for panel in lefts for x in panel], LEFT).T
        right = cat(
            [
                stack_parts([x for r, i in updates for x in (r, -i)], RIGHT),
                stack_parts([x for r, i in updates for x in (i, r)], RIGHT),
            ],
            1,
        )
        if ahead is not None:
            early = dot(left[follow : follow + span, :], right)
            window = [ahead]
            for n in range(1, GROUP):
                at = slice(ROWS * n, ROWS * (n + 1))
                r, i = load(follow + ROWS * n)
                window.append((r - early[at, 0:LANES], i - early[at, LANES:]))
        prod = dot(left, right)
        re_ref[k, :, :] = re_ref[k, :, :] - prod[:, 0:LANES]
        im_ref[k, :, :] = im_ref[k, :, :] - prod[:, LANES:]


def main_kernel(buf_ref, atom_ref, energy_ref, scale_ref, out_ref, re_ref, im_ref, pt_ref, rows_ref, acc_ref, out_tmp):
    freq = lax.axis_index("freq")
    omega = (2.0 * freq.astype(f32) + 1.0) * math.pi * BETA_INV

    atom = atom_ref[...]
    base = (atom >> 1) * 16 + (atom & 1) * 5
    lane_row = lax.broadcasted_iota(jnp.int32, (1, LANES), 1)
    target = jnp.concatenate([base + o for o in range(ORBS)] + [(lane_row >> 1) * 16 + 10], axis=1)
    pick = (lax.broadcasted_iota(jnp.int32, (1024, 768), 0) == target).astype(f32).astype(bf16)
    turned = lax.dot_general(
        buf_ref[...], pick, (((0,), (0,)), ((), ())), preferred_element_type=f32
    )
    proj_t = [turned[:, LANES * o : LANES * (o + 1)] for o in range(ORBS)]
    sig_parts = turned[0:128, 640:768] + turned[128:256, 640:768] + turned[256:384, 640:768]
    odd = (lax.broadcasted_iota(jnp.int32, (64, LANES), 1) & 1) == 1
    sig = jnp.where(odd, sig_parts[64:128, :], sig_parts[0:64, :])

    pt_ref[...] = turned[:, 0:640].astype(bf16)
    proj_b = pt_ref[...]
    for x in range(2):
        for m in range(ORBS):
            acc = None
            for o in range(ORBS):
                i = x * 25 + m * 5 + o
                term = sig[i : i + 1, :] * proj_t[o]
                acc = term if acc is None else acc + term
            rows_ref[x * BANDS : (x + 1) * BANDS, LANES * m : LANES * (m + 1)] = acc.astype(bf16)
    ups = lax.dot_general(
        rows_ref[...], proj_b, (((1,), (1,)), ((), ())), preferred_element_type=f32
    )
    up_r, up_i = ups[0:BANDS, :], ups[BANDS : 2 * BANDS, :]
    ii = lax.broadcasted_iota(jnp.int32, (BANDS, BANDS), 0)
    jj = lax.broadcasted_iota(jnp.int32, (BANDS, BANDS), 1)
    x_mat = jnp.where(ii == jj, -energy_ref[...], 0.0) - 0.5 * (up_r + up_r.T)
    y_mat = jnp.where(ii == jj, omega, 0.0) - 0.5 * (up_i + up_i.T)

    def block(i, j):
        at = (slice(LANES * i, LANES * (i + 1)), slice(LANES * j, LANES * (j + 1)))
        return x_mat[at], y_mat[at]

    sub_iota = lax.broadcasted_iota(jnp.int32, (ROWS, LANES), 0)
    lane_iota = lax.broadcasted_iota(jnp.int32, (ROWS, LANES), 1)
    zero = jnp.broadcast_to(energy_ref[:, 0:LANES] * 0.0, (ROWS, LANES))

    blocks = {(i, j): block(i, j) for i in range(CHUNKS) for j in range(CHUNKS)}
    exact = pt_ref[0:LANES, :]
    for k in range(CHUNKS):
        re_ref[k, :, :], im_ref[k, :, :] = blocks[k, k]
        sweep_block(re_ref, im_ref, k, sub_iota, lane_iota, zero)
        swept = re_ref[k, :, :], im_ref[k, :, :]
        after = range(k + 1, CHUNKS)
        stack = [swept]
        if k + 1 < CHUNKS:
            below = tuple(cat([blocks[i, k][x] for i in after], 0) for x in range(2))
            low = mul_wide(below, swept)
            for j in after:
                change = mul_wide(low, blocks[k, j])
                for i in after:
                    at = slice(LANES * (i - k - 1), LANES * (i - k))
                    blocks[i, j] = add(blocks[i, j], (change[0][at, :], change[1][at, :]))
            stack.append(low)
        lhs = tuple(cat([part[x] for part in stack], 0) for x in range(2))
        wide = mul_real(lhs, exact) if k == 0 else mul_tall(lhs, y[k])
        z = wide[0][0:LANES, :], wide[1][0:LANES, :]
        if k == 0:
            y = [[pt_ref[LANES * i : LANES * (i + 1), :].astype(f32), None] for i in range(CHUNKS)]
        for i in after:
            at = slice(LANES * (i - k), LANES * (i - k + 1))
            y[i] = [y[i][0] + wide[0][at, :], wide[1][at, :] if y[i][1] is None else y[i][1] + wide[1][at, :]]
        n = 0
        for m in range(ORBS):
            for o in range(m, ORBS):
                lm, lo = slice(LANES * m, LANES * (m + 1)), slice(LANES * o, LANES * (o + 1))
                re, im = y[k][0][:, lm] * z[0][:, lo], y[k][0][:, lm] * z[1][:, lo]
                if y[k][1] is not None:
                    re = re - y[k][1][:, lm] * z[1][:, lo]
                    im = im + y[k][1][:, lm] * z[0][:, lo]
                for x, val in ((0, re), (1, im)):
                    val = tree([val[ROWS * r : ROWS * (r + 1), :] for r in range(LANES // ROWS)])
                    at = slice(ROWS * (x * PAIRS + n), ROWS * (x * PAIRS + n + 1))
                    acc_ref[at, :] = val if k == 0 else acc_ref[at, :] + val
                n += 1
    scale = scale_ref[...]
    out_tmp[...] = jnp.zeros_like(out_tmp)
    for x in range(2):
        n = 0
        for m in range(ORBS):
            for o in range(m, ORBS):
                at = slice(ROWS * (x * PAIRS + n), ROWS * (x * PAIRS + n + 1))
                val = jnp.sum(acc_ref[at, :], axis=0, keepdims=True) * scale
                n += 1
                for i in {x * 25 + m * 5 + o, x * 25 + o * 5 + m}:
                    out_tmp[i : i + 1, :] = val
    out_ref[...] = out_tmp[...].T


def vmem():
    return pl.BlockSpec(memory_space=pltpu.VMEM)


def local(band_energy, projector, sigma, atom_of_slot, kweight):
    anywhere = pl.BlockSpec(memory_space=pltpu.HBM)
    packed, atom, energy, scale = pl.pallas_call(
        pack_kernel,
        out_shape=(
            jax.ShapeDtypeStruct((64, 16, BANDS), bf16),
            jax.ShapeDtypeStruct((1, ATOMS), jnp.int32),
            jax.ShapeDtypeStruct((1, BANDS), f32),
            jax.ShapeDtypeStruct((1, LANES), f32),
        ),
        in_specs=[anywhere] * 5,
        out_specs=(vmem(),) * 4,
        scratch_shapes=[
            pltpu.VMEM((10, BANDS), bf16),
            pltpu.VMEM((PARTS, 2, 64), f32),
            pltpu.SMEM((2,), jnp.int32),
            pltpu.VMEM((LANES, LANES), f32),
            pltpu.SemaphoreType.DMA((5,)),
        ],
        compiler_params=pltpu.CompilerParams(vmem_limit_bytes=8 * 2**20),
        name="pack",
    )(
        *(
            pltpu.with_memory_space_constraint(x, pltpu.HBM)
            for x in (
                projector.reshape(10, BANDS), sigma.reshape(PARTS, 2, 64), atom_of_slot.reshape(1, ATOMS),
                band_energy, kweight,
            )
        )
    )
    arrived = lax.all_to_all(packed, "freq", split_axis=0, concat_axis=0, tiled=True)
    blocks = pl.pallas_call(
        main_kernel,
        out_shape=jax.ShapeDtypeStruct((ATOMS, LANES), f32),
        in_specs=[vmem()] * 4,
        out_specs=vmem(),
        scratch_shapes=[
            pltpu.VMEM((CHUNKS, LANES, LANES), f32),
            pltpu.VMEM((CHUNKS, LANES, LANES), f32),
            pltpu.VMEM((BANDS, 640), bf16),
            pltpu.VMEM((2 * BANDS, 640), bf16),
            pltpu.VMEM((2 * PAIRS * ROWS, LANES), f32),
            pltpu.VMEM((LANES, LANES), f32),
        ],
        compiler_params=pltpu.CompilerParams(vmem_limit_bytes=24 * 2**20),
        name="green",
    )(arrived.reshape(1024, BANDS), atom, energy, scale)
    back = lax.all_to_all(
        blocks.reshape(ATOMS, 1, LANES), ("freq", "kpt"), split_axis=0, concat_axis=0, tiled=True
    )
    out = pl.pallas_call(
        unpack_kernel,
        out_shape=jax.ShapeDtypeStruct((PARTS, 1, 64), f32),
        in_specs=[vmem()],
        out_specs=vmem(),
        compiler_params=pltpu.CompilerParams(vmem_limit_bytes=8 * 2**20),
        name="unpack",
    )(back.reshape(ATOMS, LANES))
    return out.reshape(2, ORBS, ORBS, 1, 64)


def solution(mesh):
    placed = (P("kpt", None), P("kpt", "freq", None), P(None, None, None, "freq", None), P(), P())
    return jax.shard_map(
        local,
        mesh=mesh,
        in_specs=placed,
        out_specs=P(None, None, None, ("freq", "kpt"), None),
        check_vma=False,
    )
```

```python
import math

import jax
import jax.numpy as jnp
from jax import lax
from jax.experimental import pallas as pl
from jax.experimental.pallas import tpu as pltpu
from jax.sharding import PartitionSpec as P

BANDS = 384
ATOMS = 128
ORBS = 5
PARTS = 2 * ORBS * ORBS
BETA_INV = 0.1
LANES = 128
CHUNKS = BANDS // LANES
ROWS = 8
GROUP = 1
PAIRS = 15

f32 = jnp.float32
bf16 = jnp.bfloat16


def split3(x):
    hi = x.astype(bf16)
    rest = x - hi.astype(f32)
    mid = rest.astype(bf16)
    low = (rest - mid.astype(f32)).astype(bf16)
    return hi, mid, low


def pack_kernel(
    proj_hbm, sig_hbm, atom_hbm, energy_hbm, weight_hbm,
    out_ref, atom_ref, energy_ref, scale_ref,
    proj_ref, sig_ref, weight_ref, tmp_ref, sems,
):
    pairs = (
        (sig_hbm, sig_ref), (proj_hbm, proj_ref), (atom_hbm, atom_ref),
        (energy_hbm, energy_ref), (weight_hbm, weight_ref),
    )
    copies = [pltpu.make_async_copy(src, dst, sems.at[i]) for i, (src, dst) in enumerate(pairs)]
    for copy in copies:
        copy.start()
    for copy in copies:
        copy.wait()
    total = (weight_ref[0] + weight_ref[1]).astype(f32)
    own = jnp.where(lax.axis_index("kpt") == 0, weight_ref[0], weight_ref[1]).astype(f32)
    scale_ref[...] = jnp.full((1, LANES), -own, f32) / jnp.full((1, LANES), total, f32)
    tmp_ref[...] = jnp.zeros_like(tmp_ref)
    tmp_ref[0:PARTS, 0:64] = sig_ref[:, 0, :]
    tmp_ref[64 : 64 + PARTS, 0:64] = sig_ref[:, 1, :]
    turned = tmp_ref[...].T
    hi, mid, low = split3(turned)
    parts = [hi.astype(f32), mid.astype(f32), low.astype(f32)]
    rows = lax.broadcasted_iota(jnp.int32, (16, LANES), 0)
    base = [
        jnp.concatenate(
            [proj_ref[:, LANES * c : LANES * (c + 1)].astype(f32), jnp.zeros((6, LANES), f32)], axis=0
        )
        for c in range(3)
    ]
    for n in range(64):
        for c in range(3):
            row = jnp.broadcast_to(parts[c][n : n + 1, :], (16, LANES))
            out_ref[n, :, LANES * c : LANES * (c + 1)] = jnp.where(rows == 10, row, base[c]).astype(bf16)


def unpack_kernel(in_ref, out_ref):
    both = in_ref[pl.ds(0, 64, stride=2), :] + in_ref[pl.ds(1, 64, stride=2), :]
    turned = both.T
    for i in range(PARTS):
        out_ref[i, :, :] = turned[i : i + 1, :]


def cmul(ar, ai, br, bi):
    return ar * br - ai * bi, ar * bi + ai * br


def row_of(x, i):
    return jnp.broadcast_to(x[i : i + 1, :], (ROWS, LANES))


def lane_of(x, i, zero):
    return jnp.broadcast_to(x[:, i : i + 1], (ROWS, LANES)) + zero


def sweep_panel(panel, off, sub_iota, lane_iota, zero):
    cols = [(lane_of(panel[0], off + t, zero), lane_of(panel[1], off + t, zero)) for t in range(ROWS)]
    in_block = (lane_iota >= off) & (lane_iota < off + ROWS)
    eye = jnp.where(lane_iota == sub_iota + off, 1.0, 0.0).astype(f32)
    work = (jnp.where(in_block, eye, panel[0]), jnp.where(in_block, 0.0, panel[1]))
    for p in range(0, ROWS, 2):
        q = p + 1
        ar, ai = row_of(cols[p][0], p), row_of(cols[p][1], p)
        br, bi = row_of(cols[q][0], p), row_of(cols[q][1], p)
        dr, di = row_of(cols[q][0], q), row_of(cols[q][1], q)
        adr, adi = cmul(ar, ai, dr, di)
        bbr, bbi = cmul(br, bi, br, bi)
        det_r, det_i = adr - bbr, adi - bbi
        inv = 1.0 / (det_r * det_r + det_i * det_i)
        vr, vi = det_r * inv, -(det_i * inv)
        w11 = cmul(dr, di, vr, vi)
        w22 = cmul(ar, ai, vr, vi)
        w12 = cmul(-br, -bi, vr, vi)
        cpr, cpi = cols[p]
        cqr, cqi = cols[q]
        t1, t2 = cmul(cpr, cpi, *w11), cmul(cqr, cqi, *w12)
        t3, t4 = cmul(cpr, cpi, *w12), cmul(cqr, cqi, *w22)
        at_p, at_q = sub_iota == p, sub_iota == q
        fp = [jnp.where(at_p, -w11[z], jnp.where(at_q, -w12[z], t1[z] + t2[z])) for z in range(2)]
        fq = [jnp.where(at_p, -w12[z], jnp.where(at_q, -w22[z], t3[z] + t4[z])) for z in range(2)]
        keep = ~(at_p | at_q)

        def step(x):
            xr, xi = x
            pr, pi = row_of(xr, p), row_of(xi, p)
            qr, qi = row_of(xr, q), row_of(xi, q)
            yr = jnp.where(keep, xr, 0.0) - (fp[0] * pr - fp[1] * pi) - (fq[0] * qr - fq[1] * qi)
            yi = jnp.where(keep, xi, 0.0) - (fp[0] * pi + fp[1] * pr) - (fq[0] * qi + fq[1] * qr)
            return yr, yi

        for t in range(q + 1, ROWS):
            cols[t] = step(cols[t])
        work = step(work)
    re, im = work
    update = (jnp.where(in_block, eye - re, re), jnp.where(in_block, -im, im))
    final = (jnp.where(in_block, -re, re), jnp.where(in_block, -im, im))
    return update, final


def apply_sweep(panel, update, off):
    xr, xi = panel
    sum_r, sum_i = [], []
    for t in range(ROWS):
        cr = jnp.broadcast_to(panel[0][:, off + t : off + t + 1], (ROWS, LANES))
        ci = jnp.broadcast_to(panel[1][:, off + t : off + t + 1], (ROWS, LANES))
        ur, ui = row_of(update[0], t), row_of(update[1], t)
        pr, pi = cmul(cr, ci, ur, ui)
        sum_r.append(pr)
        sum_i.append(pi)
    return xr - tree(sum_r), xi - tree(sum_i)


def tree(terms):
    while len(terms) > 1:
        terms = [sum(terms[i : i + 2][1:], terms[i]) for i in range(0, len(terms), 2)]
    return terms[0]


LEFT = (0, 0, 1)
RIGHT = (0, 1, 0)


def cat(parts, axis):
    return jnp.concatenate(parts, axis=axis)


def dot(a, b):
    return jnp.dot(a, b, preferred_element_type=f32)


def stack_parts(rows, order):
    parts = split3(cat(rows, 0))
    return cat([parts[i] for i in order], 0)


def mul_wide(a, b):
    ar, ai = split3(a[0]), split3(a[1])
    br, bi, bn = split3(b[0]), split3(b[1]), split3(-b[1])
    left = cat([x for i in LEFT for x in (ar[i], ai[i])], 1)
    right = cat([cat([cat([br[i], bi[i]], 1), cat([bn[i], br[i]], 1)], 0) for i in RIGHT], 0)
    out = dot(left, right)
    n = b[0].shape[1]
    return out[:, 0:n], out[:, n:]


def mul_tall(a, b):
    ar, ai, an = split3(a[0]), split3(a[1]), split3(-a[1])
    br, bi = split3(b[0]), split3(b[1])
    left = cat([cat([cat([ar[i], an[i]], 1), cat([ai[i], ar[i]], 1)], 0) for i in LEFT], 1)
    right = cat([x for i in RIGHT for x in (br[i], bi[i])], 0)
    out = dot(left, right)
    m = a[0].shape[0]
    return out[0:m, :], out[m:, :]


def mul_real(a, exact):
    left = cat(split3(cat([a[0], a[1]], 0)), 1)
    out = dot(left, cat([exact] * 3, 0))
    m = a[0].shape[0]
    return out[0:m, :], out[m:, :]


def add(x, y):
    return x[0] + y[0], x[1] + y[1]


def sweep_block(re_ref, im_ref, k, sub_iota, lane_iota, zero):
    def load(off):
        return re_ref[k, off : off + ROWS, :], im_ref[k, off : off + ROWS, :]

    def masked(panel, off, stop):
        gone = (lane_iota >= off) & (lane_iota < stop)
        return jnp.where(gone, 0.0, panel[0]), jnp.where(gone, 0.0, panel[1])

    span = GROUP * ROWS
    window = [load(ROWS * n) for n in range(GROUP)]
    for base in range(0, LANES, span):
        follow = base + span
        ahead = load(follow) if follow < LANES else None
        lefts, updates = [], []
        for n in range(GROUP):
            off = base + ROWS * n
            update, final = sweep_panel(window[n], off, sub_iota, lane_iota, zero)
            re_ref[k, off : off + ROWS, :] = final[0]
            im_ref[k, off : off + ROWS, :] = final[1]
            lefts.append(masked(window[n], off, follow))
            updates.append(update)
            for m in range(n + 1, GROUP):
                window[m] = apply_sweep(window[m], update, off)
            if ahead is not None:
                ahead = apply_sweep(ahead, update, off)
        left = stack_parts([x for panel in lefts for x in panel], LEFT).T
        right = cat(
            [
                stack_parts([x for r, i in updates for x in (r, -i)], RIGHT),
                stack_parts([x for r, i in updates for x in (i, r)], RIGHT),
            ],
            1,
        )
        if ahead is not None:
            early = None
            window = [ahead]
            for n in range(1, GROUP):
                at = slice(ROWS * n, ROWS * (n + 1))
                r, i = load(follow + ROWS * n)
                window.append((r - early[at, 0:LANES], i - early[at, LANES:]))
        prod = dot(left, right)
        re_ref[k, :, :] = re_ref[k, :, :] - prod[:, 0:LANES]
        im_ref[k, :, :] = im_ref[k, :, :] - prod[:, LANES:]


def main_kernel(buf_ref, atom_ref, energy_ref, scale_ref, out_ref, re_ref, im_ref, pt_ref, rows_ref, acc_ref, out_tmp):
    freq = lax.axis_index("freq")
    omega = (2.0 * freq.astype(f32) + 1.0) * math.pi * BETA_INV

    atom = atom_ref[...]
    base = (atom >> 1) * 16 + (atom & 1) * 5
    lane_row = lax.broadcasted_iota(jnp.int32, (1, LANES), 1)
    target = jnp.concatenate([base + o for o in range(ORBS)] + [(lane_row >> 1) * 16 + 10], axis=1)
    pick = (lax.broadcasted_iota(jnp.int32, (1024, 768), 0) == target).astype(f32).astype(bf16)
    turned = lax.dot_general(
        buf_ref[...], pick, (((0,), (0,)), ((), ())), preferred_element_type=f32
    )
    proj_t = [turned[:, LANES * o : LANES * (o + 1)] for o in range(ORBS)]
    sig_parts = turned[0:128, 640:768] + turned[128:256, 640:768] + turned[256:384, 640:768]
    odd = (lax.broadcasted_iota(jnp.int32, (64, LANES), 1) & 1) == 1
    sig = jnp.where(odd, sig_parts[64:128, :], sig_parts[0:64, :])

    pt_ref[...] = turned[:, 0:640].astype(bf16)
    proj_b = pt_ref[...]
    for x in range(2):
        for m in range(ORBS):
            acc = None
            for o in range(ORBS):
                i = x * 25 + m * 5 + o
                term = sig[i : i + 1, :] * proj_t[o]
                acc = term if acc is None else acc + term
            rows_ref[x * BANDS : (x + 1) * BANDS, LANES * m : LANES * (m + 1)] = acc.astype(bf16)
    ups = lax.dot_general(
        rows_ref[...], proj_b, (((1,), (1,)), ((), ())), preferred_element_type=f32
    )
    up_r, up_i = ups[0:BANDS, :], ups[BANDS : 2 * BANDS, :]
    ii = lax.broadcasted_iota(jnp.int32, (BANDS, BANDS), 0)
    jj = lax.broadcasted_iota(jnp.int32, (BANDS, BANDS), 1)
    x_mat = jnp.where(ii == jj, -energy_ref[...], 0.0) - 0.5 * (up_r + up_r.T)
    y_mat = jnp.where(ii == jj, omega, 0.0) - 0.5 * (up_i + up_i.T)

    def block(i, j):
        at = (slice(LANES * i, LANES * (i + 1)), slice(LANES * j, LANES * (j + 1)))
        return x_mat[at], y_mat[at]

    sub_iota = lax.broadcasted_iota(jnp.int32, (ROWS, LANES), 0)
    lane_iota = lax.broadcasted_iota(jnp.int32, (ROWS, LANES), 1)
    zero = jnp.broadcast_to(energy_ref[:, 0:LANES] * 0.0, (ROWS, LANES))

    blocks = {(i, j): block(i, j) for i in range(CHUNKS) for j in range(CHUNKS)}
    exact = pt_ref[0:LANES, :]
    for k in range(CHUNKS):
        re_ref[k, :, :], im_ref[k, :, :] = blocks[k, k]
        sweep_block(re_ref, im_ref, k, sub_iota, lane_iota, zero)
        swept = re_ref[k, :, :], im_ref[k, :, :]
        after = range(k + 1, CHUNKS)
        stack = [swept]
        if k + 1 < CHUNKS:
            below = tuple(cat([blocks[i, k][x] for i in after], 0) for x in range(2))
            low = mul_wide(below, swept)
            for j in after:
                change = mul_wide(low, blocks[k, j])
                for i in after:
                    at = slice(LANES * (i - k - 1), LANES * (i - k))
                    blocks[i, j] = add(blocks[i, j], (change[0][at, :], change[1][at, :]))
            stack.append(low)
        lhs = tuple(cat([part[x] for part in stack], 0) for x in range(2))
        wide = mul_real(lhs, exact) if k == 0 else mul_tall(lhs, y[k])
        z = wide[0][0:LANES, :], wide[1][0:LANES, :]
        if k == 0:
            y = [[pt_ref[LANES * i : LANES * (i + 1), :].astype(f32), None] for i in range(CHUNKS)]
        for i in after:
            at = slice(LANES * (i - k), LANES * (i - k + 1))
            y[i] = [y[i][0] + wide[0][at, :], wide[1][at, :] if y[i][1] is None else y[i][1] + wide[1][at, :]]
        n = 0
        for m in range(ORBS):
            for o in range(m, ORBS):
                lm, lo = slice(LANES * m, LANES * (m + 1)), slice(LANES * o, LANES * (o + 1))
                re, im = y[k][0][:, lm] * z[0][:, lo], y[k][0][:, lm] * z[1][:, lo]
                if y[k][1] is not None:
                    re = re - y[k][1][:, lm] * z[1][:, lo]
                    im = im + y[k][1][:, lm] * z[0][:, lo]
                for x, val in ((0, re), (1, im)):
                    val = tree([val[ROWS * r : ROWS * (r + 1), :] for r in range(LANES // ROWS)])
                    at = slice(ROWS * (x * PAIRS + n), ROWS * (x * PAIRS + n + 1))
                    acc_ref[at, :] = val if k == 0 else acc_ref[at, :] + val
                n += 1
    scale = scale_ref[...]
    out_tmp[...] = jnp.zeros_like(out_tmp)
    for x in range(2):
        n = 0
        for m in range(ORBS):
            for o in range(m, ORBS):
                at = slice(ROWS * (x * PAIRS + n), ROWS * (x * PAIRS + n + 1))
                val = jnp.sum(acc_ref[at, :], axis=0, keepdims=True) * scale
                n += 1
                for i in {x * 25 + m * 5 + o, x * 25 + o * 5 + m}:
                    out_tmp[i : i + 1, :] = val
    out_ref[...] = out_tmp[...].T


def vmem():
    return pl.BlockSpec(memory_space=pltpu.VMEM)


def local(band_energy, projector, sigma, atom_of_slot, kweight):
    anywhere = pl.BlockSpec(memory_space=pltpu.HBM)
    packed, atom, energy, scale = pl.pallas_call(
        pack_kernel,
        out_shape=(
            jax.ShapeDtypeStruct((64, 16, BANDS), bf16),
            jax.ShapeDtypeStruct((1, ATOMS), jnp.int32),
            jax.ShapeDtypeStruct((1, BANDS), f32),
            jax.ShapeDtypeStruct((1, LANES), f32),
        ),
        in_specs=[anywhere] * 5,
        out_specs=(vmem(),) * 4,
        scratch_shapes=[
            pltpu.VMEM((10, BANDS), bf16),
            pltpu.VMEM((PARTS, 2, 64), f32),
            pltpu.SMEM((2,), jnp.int32),
            pltpu.VMEM((LANES, LANES), f32),
            pltpu.SemaphoreType.DMA((5,)),
        ],
        compiler_params=pltpu.CompilerParams(vmem_limit_bytes=8 * 2**20),
        name="pack",
    )(
        *(
            pltpu.with_memory_space_constraint(x, pltpu.HBM)
            for x in (
                projector.reshape(10, BANDS), sigma.reshape(PARTS, 2, 64), atom_of_slot.reshape(1, ATOMS),
                band_energy, kweight,
            )
        )
    )
    arrived = lax.all_to_all(packed, "freq", split_axis=0, concat_axis=0, tiled=True)
    blocks = pl.pallas_call(
        main_kernel,
        out_shape=jax.ShapeDtypeStruct((ATOMS, LANES), f32),
        in_specs=[vmem()] * 4,
        out_specs=vmem(),
        scratch_shapes=[
            pltpu.VMEM((CHUNKS, LANES, LANES), f32),
            pltpu.VMEM((CHUNKS, LANES, LANES), f32),
            pltpu.VMEM((BANDS, 640), bf16),
            pltpu.VMEM((2 * BANDS, 640), bf16),
            pltpu.VMEM((2 * PAIRS * ROWS, LANES), f32),
            pltpu.VMEM((LANES, LANES), f32),
        ],
        compiler_params=pltpu.CompilerParams(vmem_limit_bytes=24 * 2**20),
        name="green",
    )(arrived.reshape(1024, BANDS), atom, energy, scale)
    back = lax.all_to_all(
        blocks.reshape(ATOMS, 1, LANES), ("freq", "kpt"), split_axis=0, concat_axis=0, tiled=True
    )
    out = pl.pallas_call(
        unpack_kernel,
        out_shape=jax.ShapeDtypeStruct((PARTS, 1, 64), f32),
        in_specs=[vmem()],
        out_specs=vmem(),
        compiler_params=pltpu.CompilerParams(vmem_limit_bytes=8 * 2**20),
        name="unpack",
    )(back.reshape(ATOMS, LANES))
    return out.reshape(2, ORBS, ORBS, 1, 64)


def solution(mesh):
    placed = (P("kpt", None), P("kpt", "freq", None), P(None, None, None, "freq", None), P(), P())
    return jax.shard_map(
        local,
        mesh=mesh,
        in_specs=placed,
        out_specs=P(None, None, None, ("freq", "kpt"), None),
        check_vma=False,
    )
```

```python
import math

import jax
import jax.numpy as jnp
from jax import lax
from jax.experimental import pallas as pl
from jax.experimental.pallas import tpu as pltpu
from jax.sharding import PartitionSpec as P

BANDS = 384
ATOMS = 128
ORBS = 5
PARTS = 2 * ORBS * ORBS
BETA_INV = 0.1
LANES = 128
CHUNKS = BANDS // LANES
ROWS = 8
GROUP = 1
PAIRS = 15

f32 = jnp.float32
bf16 = jnp.bfloat16


def split3(x):
    hi = x.astype(bf16)
    rest = x - hi.astype(f32)
    mid = rest.astype(bf16)
    low = (rest - mid.astype(f32)).astype(bf16)
    return hi, mid, low


def pack_kernel(
    proj_hbm, sig_hbm, atom_hbm, energy_hbm, weight_hbm,
    out_ref, atom_ref, energy_ref, scale_ref,
    proj_ref, sig_ref, weight_ref, tmp_ref, sems,
):
    pairs = (
        (sig_hbm, sig_ref), (proj_hbm, proj_ref), (atom_hbm, atom_ref),
        (energy_hbm, energy_ref), (weight_hbm, weight_ref),
    )
    copies = [pltpu.make_async_copy(src, dst, sems.at[i]) for i, (src, dst) in enumerate(pairs)]
    for copy in copies:
        copy.start()
    tmp_ref[...] = jnp.zeros_like(tmp_ref)
    copies[0].wait()
    tmp_ref[0:PARTS, 0:64] = sig_ref[:, 0, :]
    tmp_ref[64 : 64 + PARTS, 0:64] = sig_ref[:, 1, :]
    turned = tmp_ref[...].T
    hi, mid, low = split3(turned)
    parts = [hi.astype(f32), mid.astype(f32), low.astype(f32)]
    rows = lax.broadcasted_iota(jnp.int32, (16, LANES), 0)
    copies[1].wait()
    base = [
        jnp.concatenate(
            [proj_ref[:, LANES * c : LANES * (c + 1)].astype(f32), jnp.zeros((6, LANES), f32)], axis=0
        )
        for c in range(3)
    ]
    for n in range(64):
        for c in range(3):
            row = jnp.broadcast_to(parts[c][n : n + 1, :], (16, LANES))
            out_ref[n, :, LANES * c : LANES * (c + 1)] = jnp.where(rows == 10, row, base[c]).astype(bf16)
    for copy in copies[2:]:
        copy.wait()
    total = (weight_ref[0] + weight_ref[1]).astype(f32)
    own = jnp.where(lax.axis_index("kpt") == 0, weight_ref[0], weight_ref[1]).astype(f32)
    scale_ref[...] = jnp.full((1, LANES), -own, f32) / jnp.full((1, LANES), total, f32)


def unpack_kernel(in_ref, out_ref):
    both = in_ref[pl.ds(0, 64, stride=2), :] + in_ref[pl.ds(1, 64, stride=2), :]
    turned = both.T
    for i in range(PARTS):
        out_ref[i, :, :] = turned[i : i + 1, :]


def cmul(ar, ai, br, bi):
    return ar * br - ai * bi, ar * bi + ai * br


def row_of(x, i):
    return jnp.broadcast_to(x[i : i + 1, :], (ROWS, LANES))


def lane_of(x, i, zero):
    return jnp.broadcast_to(x[:, i : i + 1], (ROWS, LANES)) + zero


def sweep_panel(panel, off, sub_iota, lane_iota, zero):
    cols = [(lane_of(panel[0], off + t, zero), lane_of(panel[1], off + t, zero)) for t in range(ROWS)]
    in_block = (lane_iota >= off) & (lane_iota < off + ROWS)
    eye = jnp.where(lane_iota == sub_iota + off, 1.0, 0.0).astype(f32)
    work = (jnp.where(in_block, eye, panel[0]), jnp.where(in_block, 0.0, panel[1]))
    for p in range(0, ROWS, 2):
        q = p + 1
        ar, ai = row_of(cols[p][0], p), row_of(cols[p][1], p)
        br, bi = row_of(cols[q][0], p), row_of(cols[q][1], p)
        dr, di = row_of(cols[q][0], q), row_of(cols[q][1], q)
        adr, adi = cmul(ar, ai, dr, di)
        bbr, bbi = cmul(br, bi, br, bi)
        det_r, det_i = adr - bbr, adi - bbi
        inv = 1.0 / (det_r * det_r + det_i * det_i)
        vr, vi = det_r * inv, -(det_i * inv)
        w11 = cmul(dr, di, vr, vi)
        w22 = cmul(ar, ai, vr, vi)
        w12 = cmul(-br, -bi, vr, vi)
        cpr, cpi = cols[p]
        cqr, cqi = cols[q]
        t1, t2 = cmul(cpr, cpi, *w11), cmul(cqr, cqi, *w12)
        t3, t4 = cmul(cpr, cpi, *w12), cmul(cqr, cqi, *w22)
        at_p, at_q = sub_iota == p, sub_iota == q
        fp = [jnp.where(at_p, -w11[z], jnp.where(at_q, -w12[z], t1[z] + t2[z])) for z in range(2)]
        fq = [jnp.where(at_p, -w12[z], jnp.where(at_q, -w22[z], t3[z] + t4[z])) for z in range(2)]
        keep = ~(at_p | at_q)

        def step(x):
            xr, xi = x
            pr, pi = row_of(xr, p), row_of(xi, p)
            qr, qi = row_of(xr, q), row_of(xi, q)
            yr = jnp.where(keep, xr, 0.0) - (fp[0] * pr - fp[1] * pi) - (fq[0] * qr - fq[1] * qi)
            yi = jnp.where(keep, xi, 0.0) - (fp[0] * pi + fp[1] * pr) - (fq[0] * qi + fq[1] * qr)
            return yr, yi

        for t in range(q + 1, ROWS):
            cols[t] = step(cols[t])
        work = step(work)
    re, im = work
    update = (jnp.where(in_block, eye - re, re), jnp.where(in_block, -im, im))
    final = (jnp.where(in_block, -re, re), jnp.where(in_block, -im, im))
    return update, final


def apply_sweep(panel, update, off):
    xr, xi = panel
    sum_r, sum_i = [], []
    for t in range(ROWS):
        cr = jnp.broadcast_to(panel[0][:, off + t : off + t + 1], (ROWS, LANES))
        ci = jnp.broadcast_to(panel[1][:, off + t : off + t + 1], (ROWS, LANES))
        ur, ui = row_of(update[0], t), row_of(update[1], t)
        pr, pi = cmul(cr, ci, ur, ui)
        sum_r.append(pr)
        sum_i.append(pi)
    return xr - tree(sum_r), xi - tree(sum_i)


def tree(terms):
    while len(terms) > 1:
        terms = [sum(terms[i : i + 2][1:], terms[i]) for i in range(0, len(terms), 2)]
    return terms[0]


LEFT = (0, 0, 1)
RIGHT = (0, 1, 0)


def cat(parts, axis):
    return jnp.concatenate(parts, axis=axis)


def dot(a, b):
    return jnp.dot(a, b, preferred_element_type=f32)


def stack_parts(rows, order):
    parts = split3(cat(rows, 0))
    return cat([parts[i] for i in order], 0)


def mul_wide(a, b):
    ar, ai = split3(a[0]), split3(a[1])
    br, bi, bn = split3(b[0]), split3(b[1]), split3(-b[1])
    left = cat([x for i in LEFT for x in (ar[i], ai[i])], 1)
    right = cat([cat([cat([br[i], bi[i]], 1), cat([bn[i], br[i]], 1)], 0) for i in RIGHT], 0)
    out = dot(left, right)
    n = b[0].shape[1]
    return out[:, 0:n], out[:, n:]


def mul_tall(a, b):
    ar, ai, an = split3(a[0]), split3(a[1]), split3(-a[1])
    br, bi = split3(b[0]), split3(b[1])
    left = cat([cat([cat([ar[i], an[i]], 1), cat([ai[i], ar[i]], 1)], 0) for i in LEFT], 1)
    right = cat([x for i in RIGHT for x in (br[i], bi[i])], 0)
    out = dot(left, right)
    m = a[0].shape[0]
    return out[0:m, :], out[m:, :]


def mul_real(a, exact):
    left = cat(split3(cat([a[0], a[1]], 0)), 1)
    out = dot(left, cat([exact] * 3, 0))
    m = a[0].shape[0]
    return out[0:m, :], out[m:, :]


def add(x, y):
    return x[0] + y[0], x[1] + y[1]


def sweep_block(re_ref, im_ref, k, sub_iota, lane_iota, zero):
    def load(off):
        return re_ref[k, off : off + ROWS, :], im_ref[k, off : off + ROWS, :]

    def masked(panel, off, stop):
        gone = (lane_iota >= off) & (lane_iota < stop)
        return jnp.where(gone, 0.0, panel[0]), jnp.where(gone, 0.0, panel[1])

    span = GROUP * ROWS
    window = [load(ROWS * n) for n in range(GROUP)]
    for base in range(0, LANES, span):
        follow = base + span
        ahead = load(follow) if follow < LANES else None
        lefts, updates = [], []
        for n in range(GROUP):
            off = base + ROWS * n
            update, final = sweep_panel(window[n], off, sub_iota, lane_iota, zero)
            re_ref[k, off : off + ROWS, :] = final[0]
            im_ref[k, off : off + ROWS, :] = final[1]
            lefts.append(masked(window[n], off, follow))
            updates.append(update)
            for m in range(n + 1, GROUP):
                window[m] = apply_sweep(window[m], update, off)
            if ahead is not None:
                ahead = apply_sweep(ahead, update, off)
        left = stack_parts([x for panel in lefts for x in panel], LEFT).T
        right = cat(
            [
                stack_parts([x for r, i in updates for x in (r, -i)], RIGHT),
                stack_parts([x for r, i in updates for x in (i, r)], RIGHT),
            ],
            1,
        )
        if ahead is not None:
            early = None
            window = [ahead]
            for n in range(1, GROUP):
                at = slice(ROWS * n, ROWS * (n + 1))
                r, i = load(follow + ROWS * n)
                window.append((r - early[at, 0:LANES], i - early[at, LANES:]))
        prod = dot(left, right)
        re_ref[k, :, :] = re_ref[k, :, :] - prod[:, 0:LANES]
        im_ref[k, :, :] = im_ref[k, :, :] - prod[:, LANES:]


def main_kernel(buf_ref, atom_ref, energy_ref, scale_ref, out_ref, re_ref, im_ref, pt_ref, rows_ref, acc_ref, out_tmp):
    freq = lax.axis_index("freq")
    omega = (2.0 * freq.astype(f32) + 1.0) * math.pi * BETA_INV

    atom = atom_ref[...]
    base = (atom >> 1) * 16 + (atom & 1) * 5
    lane_row = lax.broadcasted_iota(jnp.int32, (1, LANES), 1)
    target = jnp.concatenate([base + o for o in range(ORBS)] + [(lane_row >> 1) * 16 + 10], axis=1)
    pick = (lax.broadcasted_iota(jnp.int32, (1024, 768), 0) == target).astype(f32).astype(bf16)
    turned = lax.dot_general(
        buf_ref[...], pick, (((0,), (0,)), ((), ())), preferred_element_type=f32
    )
    proj_t = [turned[:, LANES * o : LANES * (o + 1)] for o in range(ORBS)]
    sig_parts = turned[0:128, 640:768] + turned[128:256, 640:768] + turned[256:384, 640:768]
    odd = (lax.broadcasted_iota(jnp.int32, (64, LANES), 1) & 1) == 1
    sig = jnp.where(odd, sig_parts[64:128, :], sig_parts[0:64, :])

    pt_ref[...] = turned[:, 0:640].astype(bf16)
    proj_b = pt_ref[...]
    for x in range(2):
        for m in range(ORBS):
            acc = None
            for o in range(ORBS):
                i = x * 25 + m * 5 + o
                term = sig[i : i + 1, :] * proj_t[o]
                acc = term if acc is None else acc + term
            rows_ref[x * BANDS : (x + 1) * BANDS, LANES * m : LANES * (m + 1)] = acc.astype(bf16)
    ups = lax.dot_general(
        rows_ref[...], proj_b, (((1,), (1,)), ((), ())), preferred_element_type=f32
    )
    up_r, up_i = ups[0:BANDS, :], ups[BANDS : 2 * BANDS, :]
    ii = lax.broadcasted_iota(jnp.int32, (BANDS, BANDS), 0)
    jj = lax.broadcasted_iota(jnp.int32, (BANDS, BANDS), 1)
    x_mat = jnp.where(ii == jj, -energy_ref[...], 0.0) - 0.5 * (up_r + up_r.T)
    y_mat = jnp.where(ii == jj, omega, 0.0) - 0.5 * (up_i + up_i.T)

    def block(i, j):
        at = (slice(LANES * i, LANES * (i + 1)), slice(LANES * j, LANES * (j + 1)))
        return x_mat[at], y_mat[at]

    sub_iota = lax.broadcasted_iota(jnp.int32, (ROWS, LANES), 0)
    lane_iota = lax.broadcasted_iota(jnp.int32, (ROWS, LANES), 1)
    zero = jnp.broadcast_to(energy_ref[:, 0:LANES] * 0.0, (ROWS, LANES))

    blocks = {(i, j): block(i, j) for i in range(CHUNKS) for j in range(CHUNKS)}
    exact = pt_ref[0:LANES, :]
    for k in range(CHUNKS):
        re_ref[k, :, :], im_ref[k, :, :] = blocks[k, k]
        sweep_block(re_ref, im_ref, k, sub_iota, lane_iota, zero)
        swept = re_ref[k, :, :], im_ref[k, :, :]
        after = range(k + 1, CHUNKS)
        stack = [swept]
        if k + 1 < CHUNKS:
            below = tuple(cat([blocks[i, k][x] for i in after], 0) for x in range(2))
            low = mul_wide(below, swept)
            for j in after:
                change = mul_wide(low, blocks[k, j])
                for i in after:
                    at = slice(LANES * (i - k - 1), LANES * (i - k))
                    blocks[i, j] = add(blocks[i, j], (change[0][at, :], change[1][at, :]))
            stack.append(low)
        lhs = tuple(cat([part[x] for part in stack], 0) for x in range(2))
        wide = mul_real(lhs, exact) if k == 0 else mul_tall(lhs, y[k])
        z = wide[0][0:LANES, :], wide[1][0:LANES, :]
        if k == 0:
            y = [[pt_ref[LANES * i : LANES * (i + 1), :].astype(f32), None] for i in range(CHUNKS)]
        for i in after:
            at = slice(LANES * (i - k), LANES * (i - k + 1))
            y[i] = [y[i][0] + wide[0][at, :], wide[1][at, :] if y[i][1] is None else y[i][1] + wide[1][at, :]]
        n = 0
        for m in range(ORBS):
            for o in range(m, ORBS):
                lm, lo = slice(LANES * m, LANES * (m + 1)), slice(LANES * o, LANES * (o + 1))
                re, im = y[k][0][:, lm] * z[0][:, lo], y[k][0][:, lm] * z[1][:, lo]
                if y[k][1] is not None:
                    re = re - y[k][1][:, lm] * z[1][:, lo]
                    im = im + y[k][1][:, lm] * z[0][:, lo]
                for x, val in ((0, re), (1, im)):
                    val = tree([val[ROWS * r : ROWS * (r + 1), :] for r in range(LANES // ROWS)])
                    at = slice(ROWS * (x * PAIRS + n), ROWS * (x * PAIRS + n + 1))
                    acc_ref[at, :] = val if k == 0 else acc_ref[at, :] + val
                n += 1
    scale = scale_ref[...]
    out_tmp[...] = jnp.zeros_like(out_tmp)
    for x in range(2):
        n = 0
        for m in range(ORBS):
            for o in range(m, ORBS):
                at = slice(ROWS * (x * PAIRS + n), ROWS * (x * PAIRS + n + 1))
                val = jnp.sum(acc_ref[at, :], axis=0, keepdims=True) * scale
                n += 1
                for i in {x * 25 + m * 5 + o, x * 25 + o * 5 + m}:
                    out_tmp[i : i + 1, :] = val
    out_ref[...] = out_tmp[...].T


def vmem():
    return pl.BlockSpec(memory_space=pltpu.VMEM)


def local(band_energy, projector, sigma, atom_of_slot, kweight):
    anywhere = pl.BlockSpec(memory_space=pltpu.HBM)
    packed, atom, energy, scale = pl.pallas_call(
        pack_kernel,
        out_shape=(
            jax.ShapeDtypeStruct((64, 16, BANDS), bf16),
            jax.ShapeDtypeStruct((1, ATOMS), jnp.int32),
            jax.ShapeDtypeStruct((1, BANDS), f32),
            jax.ShapeDtypeStruct((1, LANES), f32),
        ),
        in_specs=[anywhere] * 5,
        out_specs=(vmem(),) * 4,
        scratch_shapes=[
            pltpu.VMEM((10, BANDS), bf16),
            pltpu.VMEM((PARTS, 2, 64), f32),
            pltpu.SMEM((2,), jnp.int32),
            pltpu.VMEM((LANES, LANES), f32),
            pltpu.SemaphoreType.DMA((5,)),
        ],
        compiler_params=pltpu.CompilerParams(vmem_limit_bytes=8 * 2**20),
        name="pack",
    )(
        *(
            pltpu.with_memory_space_constraint(x, pltpu.HBM)
            for x in (
                projector.reshape(10, BANDS), sigma.reshape(PARTS, 2, 64), atom_of_slot.reshape(1, ATOMS),
                band_energy, kweight,
            )
        )
    )
    arrived = lax.all_to_all(packed, "freq", split_axis=0, concat_axis=0, tiled=True)
    blocks = pl.pallas_call(
        main_kernel,
        out_shape=jax.ShapeDtypeStruct((ATOMS, LANES), f32),
        in_specs=[vmem()] * 4,
        out_specs=vmem(),
        scratch_shapes=[
            pltpu.VMEM((CHUNKS, LANES, LANES), f32),
            pltpu.VMEM((CHUNKS, LANES, LANES), f32),
            pltpu.VMEM((BANDS, 640), bf16),
            pltpu.VMEM((2 * BANDS, 640), bf16),
            pltpu.VMEM((2 * PAIRS * ROWS, LANES), f32),
            pltpu.VMEM((LANES, LANES), f32),
        ],
        compiler_params=pltpu.CompilerParams(vmem_limit_bytes=24 * 2**20),
        name="green",
    )(arrived.reshape(1024, BANDS), atom, energy, scale)
    back = lax.all_to_all(
        blocks.reshape(ATOMS, 1, LANES), ("freq", "kpt"), split_axis=0, concat_axis=0, tiled=True
    )
    out = pl.pallas_call(
        unpack_kernel,
        out_shape=jax.ShapeDtypeStruct((PARTS, 1, 64), f32),
        in_specs=[vmem()],
        out_specs=vmem(),
        compiler_params=pltpu.CompilerParams(vmem_limit_bytes=8 * 2**20),
        name="unpack",
    )(back.reshape(ATOMS, LANES))
    return out.reshape(2, ORBS, ORBS, 1, 64)


def solution(mesh):
    placed = (P("kpt", None), P("kpt", "freq", None), P(None, None, None, "freq", None), P(), P())
    return jax.shard_map(
        local,
        mesh=mesh,
        in_specs=placed,
        out_specs=P(None, None, None, ("freq", "kpt"), None),
        check_vma=False,
    )
```
